128 devices in a mesh: row: 8 (over x, core), col: 16 (over z, y).
Axes of the slice: x: 4, y: 4, z: 4, core: 2. Of those that a mesh axis runs over, the one named last changes fastest.
Arguments:
- coords: float32 [3, 2097152], P(None, ('row', 'col')), may hold values from 0 to 6
- vectors: bfloat16 [64, 2097152], P(None, ('row', 'col')), may hold values from -0.59765625 to 0.59765625
- basis: bfloat16 [32, 2097152], P(None, ('row', 'col')), may hold values from -1.5 to 1.5
- transfer: float32 [32, 262144], P(None, ('row', 'col')), may hold values from -0.3 to 0.3
- leaf_skeleton: float32 [3, 262144], P(None, ('row', 'col')), may hold values from 0 to 6
- device_skeleton: float32 [3, 4096], P(None, ('row', 'col')), may hold values from 0 to 6
- near_pairs: int32 [2, 49152], P(None, ('row', 'col')), may hold values from 0 to 8191, as said below
- far_leaves: int32 [8192, 8], P(('row', 'col')), may hold values from 0 to 8191, as said below
- far_devices: int32 [128, 16], P(('row', 'col')), may hold values from 0 to 127
Outputs:
- product: float32 [64, 2097152], P(None, ('row', 'col'))
The draws below stay inside these ranges and needn't reach their ends.
Inputs may be any that keep to these rules, and one draw needn't show every extreme that they name: `near_pairs`: device k of the row x col grid (k = row index * 16 + col index) holds near blocks k * 6 * 64 to (k + 1) * 6 * 64 - 1 and leaves k * 64 to (k + 1) * 64 - 1; the target and the source leaf of each of its near blocks lie on device k or on a device beside it in the grid, diagonals included. `far_leaves`: the coupling partners of a leaf lie on that leaf's device or on a device beside it in the row x col grid, diagonals included.
All inputs are finite; a program needn't handle non-finite values.
Results may differ from the reference program's by a relative error of at most 0.004.
Values may be sent and summed in bfloat16 or wider, within the bound.
A program may use at most 256 MiB of HBM per device.

```python
import jax
import jax.numpy as jnp
from jax import lax

LEAF = 256
RANK = 32
VEC = 64
LEAF_DEV = 64
NEAR = 6
FAR_LEAF = 8
FAR_DEV = 16
NLEAF = 8192
NPTS = 2097152
NBLK = 49152
N_ROW = 8
N_COL = 16


def neighbour_leaf(key, owner_dev, stay, crowded):
    key_row = jax.random.fold_in(key, 1)
    key_col = jax.random.fold_in(key, 2)
    key_first = jax.random.fold_in(key, 3)
    key_second = jax.random.fold_in(key, 4)
    count = owner_dev.shape
    row_here = owner_dev // N_COL
    col_here = owner_dev % N_COL
    row_there = jnp.clip(row_here + jax.random.randint(key_row, count, -1, 2), 0, N_ROW - 1)
    col_there = jnp.clip(col_here + jax.random.randint(key_col, count, -1, 2), 0, N_COL - 1)
    row_there = jnp.where(stay > 0, row_here, row_there)
    col_there = jnp.where(stay > 0, col_here, col_there)
    leaf_first = jax.random.randint(key_first, count, 0, LEAF_DEV)
    if crowded:
        leaf_second = jax.random.randint(key_second, count, 0, LEAF_DEV)
        leaf_first = jnp.minimum(leaf_first, leaf_second)
    return (row_there * N_COL + col_there) * LEAF_DEV + leaf_first


def draw_near_pairs(key, part):
    block_dev = jnp.arange(NBLK, dtype=jnp.int32) // (NEAR * LEAF_DEV)
    stay = jax.random.randint(jax.random.fold_in(key, 13), (NBLK,), 0, 2)
    target = neighbour_leaf(jax.random.fold_in(key, 11), block_dev, stay, True)
    source = neighbour_leaf(jax.random.fold_in(key, 12), block_dev, jnp.zeros_like(stay), False)
    return jnp.stack([target, source]).astype(jnp.int32)


def draw_far_leaves(key, part):
    leaf_dev = jnp.arange(NLEAF * FAR_LEAF, dtype=jnp.int32) // (FAR_LEAF * LEAF_DEV)
    stay = jnp.zeros_like(leaf_dev)
    chosen = neighbour_leaf(jax.random.fold_in(key, 21), leaf_dev, stay, False)
    return chosen.reshape(NLEAF, FAR_LEAF).astype(jnp.int32)


def touch_ends(array, rng, smallest, largest):
    extent = array.shape
    place = [jax.random.randint(jax.random.fold_in(rng, axis), (), 0, extent[axis]) for axis in range(len(extent))]
    array = array.at[tuple(place)].set(smallest)
    longest = extent.index(max(extent))
    place[longest] = (place[longest] + 1) % extent[longest]
    return array.at[tuple(place)].set(largest)


def shard_levels(stream_key, dims, shards, low, largest):
    factor_of, own = 1.0, jax.random.fold_in(stream_key, 6)
    for position, shards_of in shards:
        draws = jnp.exp(jax.random.uniform(jax.random.fold_in(own, position), (shards_of,), jnp.float32, low / len(shards), largest / len(shards)))
        factor_of = factor_of * jnp.repeat(draws, dims[position] // shards_of).reshape([-1 if axis == position else 1 for axis in range(len(dims))])
    return factor_of


def scatter_about(key, shape, spread, reach, shards=(), kind=jnp.bfloat16):
    result = spread * jax.random.normal(key, shape, jnp.float32)
    if shards:
        result = result * shard_levels(key, shape, shards, -0.22, 0.18)
    return jnp.clip(result, -reach, reach).astype(kind)


def setup_inputs(seed: int = 0) -> dict:
    key_of = jax.random.split(jax.random.key(seed), 10)
    return {
        "coords": jnp.clip(6.0 * jax.random.uniform(key_of[0], (3, NPTS), jnp.float32) ** shard_levels(key_of[0], (3, NPTS), ((1, 128),), -0.2, 0.2), 0.0, 6.0),
        "vectors": scatter_about(key_of[1], (VEC, NPTS), 0.1, 0.59765625, ((1, 128),)),
        "basis": scatter_about(key_of[2], (RANK, NPTS), 0.25, 1.5, ((1, 128),)),
        "transfer": scatter_about(key_of[3], (RANK, NLEAF * RANK), 0.05, 0.3, ((1, 128),), jnp.float32),
        "leaf_skeleton": jnp.clip(6.0 * jax.random.uniform(key_of[4], (3, NLEAF * RANK), jnp.float32) ** shard_levels(key_of[4], (3, NLEAF * RANK), ((1, 128),), -0.2, 0.2), 0.0, 6.0),
        "device_skeleton": jnp.clip(6.0 * jax.random.uniform(key_of[5], (3, N_ROW * N_COL * RANK), jnp.float32) ** shard_levels(key_of[5], (3, N_ROW * N_COL * RANK), ((1, 128),), -0.2, 0.2), 0.0, 6.0),
        "near_pairs": draw_near_pairs(jax.random.fold_in(key_of[9], 71), 0),
        "far_leaves": draw_far_leaves(jax.random.fold_in(key_of[9], 71), 0),
        "far_devices": touch_ends(jax.random.randint(key_of[8], (N_ROW * N_COL, FAR_DEV), 0, N_ROW * N_COL), jax.random.fold_in(key_of[8], 1), 0, (N_ROW * N_COL) - 1).astype(jnp.int32),
    }


HIGH = lax.Precision.HIGHEST


def kernel_block(left, right):
    total = None
    for dimension in range(3):
        gap = left[..., dimension, :, None] - right[..., dimension, None, :]
        total = gap * gap if total is None else total + gap * gap
    return jnp.exp(-0.5 * total)


def reference(coords, vectors, basis, transfer, leaf_skeleton, device_skeleton, near_pairs, far_leaves, far_devices):
    devices = N_ROW * N_COL
    coords_leaf = coords.reshape(3, NLEAF, LEAF)
    vectors_leaf = vectors.reshape(VEC, NLEAF, LEAF)
    pairs = near_pairs.reshape(2, devices, NEAR * LEAF_DEV)

    def near_step(total, pair):
        target, source = pair
        tgt_points = jnp.transpose(coords_leaf[:, target], (1, 0, 2))
        src_points = jnp.transpose(coords_leaf[:, source], (1, 0, 2))
        block = kernel_block(tgt_points, src_points).astype(jnp.bfloat16)
        src_vectors = vectors_leaf[:, source].astype(jnp.float32)
        partial_value = jnp.einsum("vbs,bts->bvt", src_vectors, block.astype(jnp.float32), precision=HIGH)
        return total.at[target].add(partial_value), None

    start = jnp.zeros((NLEAF, VEC, LEAF), jnp.float32)
    near_total, _ = lax.scan(near_step, start, (pairs[0], pairs[1]))
    near_field = jnp.transpose(near_total, (1, 0, 2)).reshape(VEC, NPTS)

    basis_leaf = basis.reshape(RANK, NLEAF, LEAF)
    coeff = jnp.einsum("vnl,rnl->vnr", vectors_leaf.astype(jnp.float32), basis_leaf.astype(jnp.float32), precision=HIGH).astype(jnp.bfloat16)
    transfer_mats = transfer.reshape(RANK, NLEAF, RANK)
    coeff_dev = coeff.astype(jnp.float32).reshape(VEC, devices, LEAF_DEV, RANK)
    device_coeff = jnp.einsum("vdir,rdis->vds", coeff_dev, transfer_mats.reshape(RANK, devices, LEAF_DEV, RANK), precision=HIGH)

    skeleton_leaf = leaf_skeleton.reshape(3, NLEAF, RANK)

    def leaf_block(item):
        lists, own_skel = item
        picked = jnp.transpose(coeff[:, lists].astype(jnp.float32), (1, 2, 0, 3))
        picked_skel = jnp.transpose(skeleton_leaf[:, lists], (1, 2, 0, 3))
        coupling = kernel_block(picked_skel, own_skel[:, None])
        return jnp.einsum("ifvs,ifst->ivt", picked, coupling, precision=HIGH)

    own_skeleton = jnp.transpose(skeleton_leaf, (1, 0, 2)).reshape(devices, LEAF_DEV, 3, RANK)
    leaf_far = lax.map(leaf_block, (far_leaves.reshape(devices, LEAF_DEV, FAR_LEAF), own_skeleton))
    leaf_far = leaf_far.reshape(NLEAF, VEC, RANK)

    skeleton_dev = device_skeleton.reshape(3, devices, RANK)
    picked_coeff = device_coeff[:, far_devices]
    picked_skel = jnp.transpose(skeleton_dev[:, far_devices], (1, 2, 0, 3))
    own_dev_skel = jnp.transpose(skeleton_dev, (1, 0, 2))
    coupling_top = kernel_block(picked_skel, own_dev_skel[:, None])
    device_far = jnp.einsum("vdfs,dfst->dvt", picked_coeff, coupling_top, precision=HIGH)

    device_of_leaf = jnp.repeat(device_far, LEAF_DEV, axis=0)
    field = leaf_far + jnp.einsum("nvs,rns->nvr", device_of_leaf, transfer_mats, precision=HIGH)
    field = field.astype(jnp.bfloat16)
    far_part = jnp.einsum("nvr,rnl->vnl", field.astype(jnp.float32), basis_leaf.astype(jnp.float32), precision=HIGH)
    return near_field + far_part.reshape(VEC, NPTS)
```

```python
import functools
import math

import jax
import jax.numpy as jnp
from jax import lax
from jax.experimental import pallas as pl
from jax.experimental.pallas import tpu as pltpu
from jax.sharding import PartitionSpec as P

HIGH = lax.Precision.HIGHEST
F32 = jnp.float32
BF16 = jnp.bfloat16
MESH = pl.DeviceIdType.MESH
SCALE = math.sqrt(math.log2(math.e))
MIDDLE = 3.0
CHUNK = 16


def point_features(points):
    scaled = (points - MIDDLE) * SCALE
    high = lax.reduce_precision(scaled, 8, 7)
    low = lax.reduce_precision(scaled - high, 8, 7)
    whole = high + low
    norm = -0.5 * (whole[0:1] ** 2 + whole[1:2] ** 2 + whole[2:3] ** 2)
    norm_high = lax.reduce_precision(norm, 8, 7)
    return jnp.concatenate([high, norm_high, low, norm - norm_high], axis=0).astype(BF16)


def kernel_block(left, right):
    total = None
    for dimension in range(3):
        gap = left[..., dimension, :, None] - right[..., dimension, None, :]
        total = gap * gap if total is None else total + gap * gap
    return jnp.exp(-0.5 * total)


def remote(src, dst, send, recv, device):
    return pltpu.make_async_remote_copy(
        src_ref=src, dst_ref=dst, send_sem=send, recv_sem=recv, device_id=device, device_id_type=MESH
    )


def halo_kernel(
    rows, cols, vec, geo, coeff, share,
    vec_pool, geo_pool, coeff_pool, every,
    row_share, send, recv, row_send, row_recv, col_send, col_recv, local,
):
    row, col = lax.axis_index("row"), lax.axis_index("col")
    barrier = pltpu.get_barrier_semaphore()
    for d in range(1, rows):
        pl.semaphore_signal(barrier, inc=1, device_id=(lax.rem(row + d, rows), col), device_id_type=MESH)
    for d in range(1, cols):
        pl.semaphore_signal(barrier, inc=1, device_id=(row, lax.rem(col + d, cols)), device_id_type=MESH)
    pl.semaphore_wait(barrier, rows + cols - 2)

    chunks = vec.shape[0] // CHUNK
    items = chunks + 2
    order = [0, chunks, chunks + 1] + list(range(1, chunks))

    def own(item):
        if item < chunks:
            return vec.at[pl.ds(item * CHUNK, CHUNK)]
        return geo if item == chunks else coeff

    def slot(hood, item):
        if item < chunks:
            return vec_pool.at[hood, pl.ds(item * CHUNK, CHUNK)]
        return (geo_pool if item == chunks else coeff_pool).at[hood]

    def copy(src, hood, item, device):
        return remote(src, slot(hood, item), send.at[hood, item], recv.at[hood, item], device)

    has_up, has_down = row > 0, row < rows - 1
    has_left, has_right = col > 0, col < cols - 1
    up, down, left, right = (row - 1, col), (row + 1, col), (row, col - 1), (row, col + 1)

    row_copies = []
    for d in range(1, rows):
        c = remote(share, row_share.at[row], row_send.at[d], row_recv.at[d], (lax.rem(row + d, rows), col))
        c.start()
        row_copies.append(c)
    keep_share = pltpu.make_async_copy(share, row_share.at[row], local.at[0])
    keep_share.start()
    keeps = [
        pltpu.make_async_copy(vec, vec_pool.at[4], local.at[1]),
        pltpu.make_async_copy(geo, geo_pool.at[4], local.at[2]),
        pltpu.make_async_copy(coeff, coeff_pool.at[4], local.at[3]),
    ]
    for k in keeps:
        k.start()

    direct = [(has_right, right, 3), (has_left, left, 5), (has_down, down, 1), (has_up, up, 7)]
    for item in order:
        for has, device, hood in direct:
            @pl.when(has)
            def _(device=device, hood=hood, item=item):
                copy(own(item), hood, item, device).start()

    keep_share.wait()
    for c in row_copies:
        c.wait_recv()
    col_copies = []
    for d in range(1, cols):
        c = remote(row_share, every.at[col], col_send.at[d], col_recv.at[d], (row, lax.rem(col + d, cols)))
        c.start()
        col_copies.append(c)
    keep_row = pltpu.make_async_copy(row_share, every.at[col], local.at[0])
    keep_row.start()

    passed = [(3, has_left, 0, 6), (5, has_right, 2, 8)]
    for item in order:
        for hood, has, to_down, to_up in passed:
            @pl.when(has)
            def _(hood=hood, item=item, to_down=to_down, to_up=to_up):
                copy(own(item), hood, item, down).wait_recv()

                @pl.when(has_down)
                def _():
                    copy(slot(hood, item), to_down, item, down).start()

                @pl.when(has_up)
                def _():
                    copy(slot(hood, item), to_up, item, up).start()

    keep_row.wait()
    for k in keeps:
        k.wait()
    for c in col_copies:
        c.wait_recv()
    for item in order:
        for has, hood in [
            (has_up, 1), (has_down, 7),
            (has_up & has_left, 0), (has_up & has_right, 2),
            (has_down & has_left, 6), (has_down & has_right, 8),
        ]:
            @pl.when(has)
            def _(hood=hood, item=item):
                copy(own(item), hood, item, down).wait_recv()
    for item in order:
        for has, hood in [
            (has_right, 3), (has_left, 5), (has_down, 1), (has_up, 7),
            (has_down & has_left, 0), (has_up & has_left, 6),
            (has_down & has_right, 2), (has_up & has_right, 8),
        ]:
            @pl.when(has)
            def _(hood=hood, item=item):
                copy(own(item), hood, item, down).wait_send()
    for c in row_copies + col_copies:
        c.wait_send()


def exchange(rows, cols, vec, geo, coeff, share):
    chunks = vec.shape[0] // CHUNK
    vmem = pl.BlockSpec(memory_space=pltpu.VMEM)
    hbm = pl.BlockSpec(memory_space=pl.ANY)
    pool = lambda a: jax.ShapeDtypeStruct((9, *a.shape), a.dtype)
    dma = pltpu.SemaphoreType.DMA
    return pl.pallas_call(
        functools.partial(halo_kernel, rows, cols),
        out_shape=(pool(vec), pool(geo), pool(coeff), jax.ShapeDtypeStruct((cols, rows, *share.shape), F32)),
        in_specs=[vmem] * 4,
        out_specs=(hbm, hbm, hbm, vmem),
        scratch_shapes=[
            pltpu.VMEM((rows, *share.shape), F32),
            dma((9, chunks + 2)), dma((9, chunks + 2)),
            dma((rows,)), dma((rows,)), dma((cols,)), dma((cols,)), dma((4,)),
        ],
        compiler_params=pltpu.CompilerParams(
            collective_id=0, has_side_effects=True, vmem_limit_bytes=24 * 2**20
        ),
        name="halo",
    )(vec, geo, coeff, share)


GROUP = 8
RING = 32
STAGES = 4


def near_kernel(
    blocks, leaves, index, vec_pool, geo_pool,
    partial, mine, feats, vbuf, acc, stage, touched, vsem, gsem, ssem,
):
    width = vbuf.shape[2]
    count = 9 * leaves
    share = stage.shape[1]
    geo_copy = pltpu.make_async_copy(geo_pool, feats, gsem.at[0])
    geo_copy.start()

    def fetch(p, slot):
        hood, leaf = index[2, p], index[3, p]
        return pltpu.make_async_copy(
            vec_pool.at[hood, :, pl.ds(pl.multiple_of(leaf * width, width), width)], vbuf.at[slot], vsem.at[slot]
        )

    for p in range(RING):
        fetch(p, p).start()

    @pl.loop(0, count)
    def _(i):
        touched[i] = 0

    geo_copy.wait()
    row_id = lax.broadcasted_iota(jnp.int32, (8, width), 0)
    unit = lax.rem(row_id, 4) == 3

    def features(hood, leaf):
        return feats[hood, :, pl.ds(pl.multiple_of(leaf * width, width), width)].astype(F32)

    def power(p):
        tgt = features(index[0, p], index[1, p])
        src = features(index[2, p], index[3, p])
        turned = jnp.concatenate([tgt[4:8], tgt[0:4]], axis=0)
        left = jnp.concatenate([src, jnp.where(unit, 1.0, src)], axis=0).astype(BF16)
        right = jnp.concatenate(
            [
                jnp.where(unit, 1.0, jnp.where(row_id < 4, tgt, turned)),
                jnp.where(row_id < 3, turned, tgt),
            ],
            axis=0,
        ).astype(BF16)
        return lax.dot_general(left, right, (((0,), (0,)), ((), ())), preferred_element_type=F32)

    @pl.loop(0, blocks // GROUP)
    def _(step):
        first = step * GROUP
        at = lax.rem(first, RING)
        for k in range(GROUP):
            fetch(first + k, at + k).wait()
        ahead = power(first)
        for k in range(GROUP):
            now = ahead
            if k + 1 < GROUP:
                ahead = power(first + k + 1)
            part = jnp.dot(vbuf[at + k], jnp.exp2(now).astype(BF16), preferred_element_type=F32)
            place = index[0, first + k] * leaves + index[1, first + k]
            seen = touched[place]
            touched[place] = 1
            acc[place] = jnp.where(seen > 0, acc[place], 0.0) + part

        @pl.when(first + RING < blocks)
        def _():
            for k in range(GROUP):
                fetch(first + RING + k, at + k).start()

    def settle(place):
        @pl.when(touched[place] == 0)
        def _():
            acc[place] = jnp.zeros(acc.shape[1:], F32)

    @pl.loop(0, leaves)
    def _(leaf):
        settle(4 * leaves + leaf)

    put_mine = pltpu.make_async_copy(acc.at[pl.ds(4 * leaves, leaves)], mine, gsem.at[0])
    put_mine.start()

    def put(hood, part):
        return pltpu.make_async_copy(
            stage.at[lax.rem(part, STAGES)], partial.at[hood, pl.ds(part * share, share)],
            ssem.at[lax.rem(part, STAGES)],
        )

    parts = leaves // share
    for hood in [h for h in range(9) if h != 4]:
        @pl.loop(0, parts)
        def _(part, hood=hood):
            if hood == 0:
                @pl.when(part >= STAGES)
                def _():
                    put(hood, part).wait()
            else:
                put(hood, part).wait()

            @pl.loop(0, share)
            def _(k):
                place = hood * leaves + part * share + k
                slot = lax.rem(part, STAGES)

                @pl.when(touched[place] > 0)
                def _():
                    stage[slot, k] = acc[place].astype(BF16)

                @pl.when(touched[place] == 0)
                def _():
                    stage[slot, k] = jnp.zeros(stage.shape[2:], BF16)

            put(hood, part).start()

    for slot in range(STAGES):
        put(0, slot).wait()
    put_mine.wait()


def near_blocks(index, vec_pool, geo_pool, leaves, width):
    blocks = index.shape[1]
    vecs = vec_pool.shape[1]
    share = leaves // STAGES
    hbm = pl.BlockSpec(memory_space=pl.ANY)
    dma = pltpu.SemaphoreType.DMA
    return pl.pallas_call(
        functools.partial(near_kernel, blocks, leaves),
        out_shape=(
            jax.ShapeDtypeStruct((9, leaves, vecs, width), BF16),
            jax.ShapeDtypeStruct((leaves, vecs, width), F32),
        ),
        in_specs=[pl.BlockSpec(memory_space=pltpu.SMEM), hbm, hbm],
        out_specs=(hbm, hbm),
        scratch_shapes=[
            pltpu.VMEM(geo_pool.shape, BF16),
            pltpu.VMEM((RING, vecs, width), BF16),
            pltpu.VMEM((9 * leaves, vecs, width), F32),
            pltpu.VMEM((STAGES, share, vecs, width), BF16),
            pltpu.SMEM((9 * leaves,), jnp.int32),
            dma((RING,)), dma((1,)), dma((STAGES,)),
        ],
        compiler_params=pltpu.CompilerParams(vmem_limit_bytes=58 * 2**20),
        name="near",
    )(index, vec_pool, geo_pool)


def return_kernel(
    rows, cols, chunks, partial, base, out,
    from_rows, sums, from_cols, row_send, row_recv, col_send, col_recv, local,
):
    row, col = lax.axis_index("row"), lax.axis_index("col")
    has_row = (row > 0, row < rows - 1)
    has_col = (col > 0, col < cols - 1)
    leaves, vecs, width = base.shape
    share = leaves // chunks
    loads = [
        pltpu.make_async_copy(partial.at[3], sums.at[0], local.at[0]),
        pltpu.make_async_copy(partial.at[5], sums.at[1], local.at[1]),
    ]
    for c in loads:
        c.start()
    barrier = pltpu.get_barrier_semaphore()
    row_dev = ((row - 1, col), (row + 1, col))
    col_dev = ((row, col - 1), (row, col + 1))
    peers = 0
    for has, dev in zip(has_row + has_col, row_dev + col_dev):
        peers = peers + has.astype(jnp.int32)

        @pl.when(has)
        def _(dev=dev):
            pl.semaphore_signal(barrier, inc=1, device_id=dev, device_id_type=MESH)
    pl.semaphore_wait(barrier, peers)

    def some(c):
        return pl.ds(c * share, share)

    def row_copy(side, place, c):
        hood = (0 if side == 0 else 6) + (0, 2, 1)[place]
        return remote(
            partial.at[hood, some(c)], from_rows.at[1 - side, place, some(c)],
            row_send.at[side, place, c], row_recv.at[1 - side, place, c], row_dev[side],
        )

    def col_copy(side, c):
        return remote(
            sums.at[side, some(c)], from_cols.at[1 - side, some(c)],
            col_send.at[side, c], col_recv.at[1 - side, c], col_dev[side],
        )

    wanted = has_col + (True,)
    plan = [(place, c) for c in range(chunks) for place in (0, 1)] + [(2, c) for c in range(chunks)]
    for place, c in plan:
        for side in (0, 1):
            @pl.when(has_row[side] & wanted[place])
            def _(side=side, place=place, c=c):
                row_copy(side, place, c).start()

    def fill(ref):
        @pl.loop(0, leaves)
        def _(i):
            ref[i] = jnp.zeros((vecs, width), BF16)

    for side in (0, 1):
        @pl.when(jnp.logical_not(has_row[side]))
        def _(side=side):
            for place in range(3):
                fill(from_rows.at[side, place])

        @pl.when(jnp.logical_not(has_col[side]))
        def _(side=side):
            fill(from_cols.at[side])

    for c in loads:
        c.wait()

    for c in range(chunks):
        for place in (0, 1):
            @pl.when(has_col[place])
            def _(place=place, c=c):
                for side in (0, 1):
                    @pl.when(has_row[side])
                    def _(side=side):
                        row_copy(1 - side, place, c).wait_recv()

                @pl.loop(c * share, (c + 1) * share)
                def _(i):
                    total = (
                        sums[place, i].astype(F32)
                        + from_rows[0, place, i].astype(F32)
                        + from_rows[1, place, i].astype(F32)
                    )
                    sums[place, i] = total.astype(BF16)

                col_copy(place, c).start()

    for c in range(chunks):
        for side in (0, 1):
            @pl.when(has_row[side])
            def _(side=side, c=c):
                row_copy(1 - side, 2, c).wait_recv()

            @pl.when(has_col[side])
            def _(side=side, c=c):
                col_copy(1 - side, c).wait_recv()

        @pl.loop(c * share, (c + 1) * share)
        def _(i):
            out[:, pl.ds(pl.multiple_of(i * width, width), width)] = (
                base[i]
                + from_rows[0, 2, i].astype(F32)
                + from_rows[1, 2, i].astype(F32)
                + from_cols[0, i].astype(F32)
                + from_cols[1, i].astype(F32)
            )

    for place, c in plan:
        for side in (0, 1):
            @pl.when(has_row[side] & wanted[place])
            def _(side=side, place=place, c=c):
                row_copy(side, place, c).wait_send()
    for c in range(chunks):
        for side in (0, 1):
            @pl.when(has_col[side])
            def _(side=side, c=c):
                col_copy(side, c).wait_send()


def give_back(rows, cols, partial, base):
    leaves, vecs, width = base.shape
    chunks = math.gcd(leaves, 4)
    vmem = pl.BlockSpec(memory_space=pltpu.VMEM)
    dma = pltpu.SemaphoreType.DMA
    return pl.pallas_call(
        functools.partial(return_kernel, rows, cols, chunks),
        out_shape=jax.ShapeDtypeStruct((vecs, leaves * width), F32),
        in_specs=[pl.BlockSpec(memory_space=pl.ANY), vmem],
        out_specs=vmem,
        scratch_shapes=[
            pltpu.VMEM((2, 3, leaves, vecs, width), BF16),
            pltpu.VMEM((2, leaves, vecs, width), BF16),
            pltpu.VMEM((2, leaves, vecs, width), BF16),
            dma((2, 3, chunks)), dma((2, 3, chunks)), dma((2, chunks)), dma((2, chunks)), dma((2,)),
        ],
        compiler_params=pltpu.CompilerParams(
            collective_id=1, has_side_effects=True, vmem_limit_bytes=48 * 2**20
        ),
        name="give_back",
    )(partial, base)


def shards(
    coords, vectors, basis, transfer, leaf_skeleton, device_skeleton, near_pairs, far_leaves, far_devices
):
    row_count, col_count = lax.axis_size("row"), lax.axis_size("col")
    row_here, col_here = lax.axis_index("row"), lax.axis_index("col")
    rank_size, vec_count = basis.shape[0], vectors.shape[0]
    leaves = transfer.shape[1] // rank_size
    leaf_width = coords.shape[1] // leaves
    points = coords.shape[1]

    def hood_of(global_leaf):
        owner = global_leaf // leaves
        hood = (owner // col_count - row_here + 1) * 3 + (owner % col_count - col_here + 1)
        return hood, global_leaf % leaves

    geo = point_features(jnp.concatenate([coords, leaf_skeleton], axis=1))
    coeff = jnp.einsum(
        "vil,ril->irv",
        vectors.reshape(vec_count, leaves, leaf_width),
        basis.reshape(rank_size, leaves, leaf_width),
        preferred_element_type=F32,
    ).astype(BF16)
    transfer_mats = transfer.reshape(rank_size, leaves, rank_size)
    device_coeff = jnp.einsum("irv,ris->vs", coeff.astype(F32), transfer_mats, precision=HIGH)
    paired = coeff.reshape(leaves // 2, 2, rank_size, vec_count)
    paired = jnp.transpose(paired, (0, 2, 1, 3)).reshape(leaves // 2 * rank_size, 2 * vec_count)
    flat = jnp.concatenate([device_coeff.reshape(-1), device_skeleton.reshape(-1)])
    flat = jnp.pad(flat, (0, -flat.size % 1024)).reshape(-1, 128)

    vec_pool, geo_pool, coeff_pool, every = exchange(row_count, col_count, vectors, geo, paired, flat)

    t_hood, t_leaf = hood_of(near_pairs[0])
    s_hood, s_leaf = hood_of(near_pairs[1])
    index = jnp.stack([t_hood, t_leaf, s_hood, s_leaf])
    partial, mine = near_blocks(index, vec_pool, geo_pool, leaves, leaf_width)

    far_hood, far_leaf = hood_of(far_leaves)
    skel = geo_pool[:, :, points:].astype(F32)
    skel = (skel[:, 0:3] + skel[:, 4:7]).reshape(9, 3, leaves, rank_size)
    picked_skel = skel[far_hood, :, far_leaf, :]
    own_skel = jnp.transpose(skel[4], (1, 0, 2))
    total = None
    for k in range(3):
        gap = picked_skel[..., k, :, None] - own_skel[:, None, k, None, :]
        total = gap * gap if total is None else total + gap * gap
    coupling = jnp.exp2(-0.5 * total)
    coeff_all = coeff_pool.reshape(9, leaves // 2, rank_size, 2, vec_count)
    picked_coeff = coeff_all[far_hood, far_leaf // 2, :, far_leaf % 2, :].astype(F32)
    leaf_far = jnp.einsum("ifsv,ifst->ivt", picked_coeff, coupling, precision=HIGH)

    chosen = far_devices[0]
    picked = every[chosen % col_count, chosen // col_count].reshape(chosen.shape[0], -1)
    size = vec_count * rank_size
    top_coeffs = picked[:, :size].reshape(-1, vec_count, rank_size)
    top_skel = picked[:, size : size + 3 * rank_size].reshape(-1, 3, rank_size)
    coupling_top = kernel_block(top_skel, device_skeleton[None])
    device_far = jnp.einsum("fvs,fst->vt", top_coeffs, coupling_top, precision=HIGH)
    field = leaf_far + jnp.einsum("vs,ris->ivr", device_far, transfer_mats, precision=HIGH)
    far_part = jnp.einsum(
        "ivr,ril->ivl",
        field.astype(BF16),
        basis.reshape(rank_size, leaves, leaf_width),
        preferred_element_type=F32,
    )
    base = mine + far_part
    return give_back(row_count, col_count, partial, base)


def solution(mesh):
    wide = P(None, ("row", "col"))
    tall = P(("row", "col"), None)
    return jax.shard_map(
        shards, mesh=mesh, in_specs=(wide,) * 7 + (tall,) * 2, out_specs=wide, check_vma=False
    )
```

```python
import functools
import math

import jax
import jax.numpy as jnp
from jax import lax
from jax.experimental import pallas as pl
from jax.experimental.pallas import tpu as pltpu
from jax.sharding import PartitionSpec as P

HIGH = lax.Precision.HIGHEST
F32 = jnp.float32
BF16 = jnp.bfloat16
MESH = pl.DeviceIdType.MESH
SCALE = math.sqrt(math.log2(math.e))
MIDDLE = 3.0
CHUNK = 16


def point_features(points):
    scaled = (points - MIDDLE) * SCALE
    high = lax.reduce_precision(scaled, 8, 7)
    low = lax.reduce_precision(scaled - high, 8, 7)
    whole = high + low
    norm = -0.5 * (whole[0:1] ** 2 + whole[1:2] ** 2 + whole[2:3] ** 2)
    norm_high = lax.reduce_precision(norm, 8, 7)
    return jnp.concatenate([high, norm_high, low, norm - norm_high], axis=0).astype(BF16)


def remote(src, dst, send, recv, device):
    return pltpu.make_async_remote_copy(
        src_ref=src, dst_ref=dst, send_sem=send, recv_sem=recv, device_id=device, device_id_type=MESH
    )


def halo_kernel(
    rows, cols, vec, geo, coeff, share,
    vec_pool, geo_pool, coeff_pool, every,
    row_share, send, recv, row_send, row_recv, col_send, col_recv, local,
):
    row, col = lax.axis_index("row"), lax.axis_index("col")
    barrier = pltpu.get_barrier_semaphore()
    for d in range(1, rows):
        pl.semaphore_signal(barrier, inc=1, device_id=(lax.rem(row + d, rows), col), device_id_type=MESH)
    for d in range(1, cols):
        pl.semaphore_signal(barrier, inc=1, device_id=(row, lax.rem(col + d, cols)), device_id_type=MESH)
    pl.semaphore_wait(barrier, rows + cols - 2)

    chunks = vec.shape[0] // CHUNK
    items = chunks + 2
    order = [0, chunks, chunks + 1] + list(range(1, chunks))

    def own(item):
        if item < chunks:
            return vec.at[pl.ds(item * CHUNK, CHUNK)]
        return geo if item == chunks else coeff

    def slot(hood, item):
        if item < chunks:
            return vec_pool.at[hood, pl.ds(item * CHUNK, CHUNK)]
        return (geo_pool if item == chunks else coeff_pool).at[hood]

    def copy(src, hood, item, device):
        return remote(src, slot(hood, item), send.at[hood, item], recv.at[hood, item], device)

    has_up, has_down = row > 0, row < rows - 1
    has_left, has_right = col > 0, col < cols - 1
    up, down, left, right = (row - 1, col), (row + 1, col), (row, col - 1), (row, col + 1)

    row_copies = []
    for d in range(1, rows):
        c = remote(share, row_share.at[row], row_send.at[d], row_recv.at[d], (lax.rem(row + d, rows), col))
        c.start()
        row_copies.append(c)
    keep_share = pltpu.make_async_copy(share, row_share.at[row], local.at[0])
    keep_share.start()
    keeps = [
        pltpu.make_async_copy(vec, vec_pool.at[4], local.at[1]),
        pltpu.make_async_copy(geo, geo_pool.at[4], local.at[2]),
        pltpu.make_async_copy(coeff, coeff_pool.at[4], local.at[3]),
    ]
    for k in keeps:
        k.start()

    direct = [(has_right, right, 3), (has_left, left, 5), (has_down, down, 1), (has_up, up, 7)]
    for item in order:
        for has, device, hood in direct:
            @pl.when(has)
            def _(device=device, hood=hood, item=item):
                copy(own(item), hood, item, device).start()

    keep_share.wait()
    for c in row_copies:
        c.wait_recv()
    col_copies = []
    for d in range(1, cols):
        c = remote(row_share, every.at[col], col_send.at[d], col_recv.at[d], (row, lax.rem(col + d, cols)))
        c.start()
        col_copies.append(c)
    keep_row = pltpu.make_async_copy(row_share, every.at[col], local.at[0])
    keep_row.start()

    passed = [(3, has_left, 0, 6), (5, has_right, 2, 8)]
    for item in order:
        for hood, has, to_down, to_up in passed:
            @pl.when(has)
            def _(hood=hood, item=item, to_down=to_down, to_up=to_up):
                copy(own(item), hood, item, down).wait_recv()

                @pl.when(has_down)
                def _():
                    copy(slot(hood, item), to_down, item, down).start()

                @pl.when(has_up)
                def _():
                    copy(slot(hood, item), to_up, item, up).start()

    keep_row.wait()
    for k in keeps:
        k.wait()
    for c in col_copies:
        c.wait_recv()
    for item in order:
        for has, hood in [
            (has_up, 1), (has_down, 7),
            (has_up & has_left, 0), (has_up & has_right, 2),
            (has_down & has_left, 6), (has_down & has_right, 8),
        ]:
            @pl.when(has)
            def _(hood=hood, item=item):
                copy(own(item), hood, item, down).wait_recv()
    for item in order:
        for has, hood in [
            (has_right, 3), (has_left, 5), (has_down, 1), (has_up, 7),
            (has_down & has_left, 0), (has_up & has_left, 6),
            (has_down & has_right, 2), (has_up & has_right, 8),
        ]:
            @pl.when(has)
            def _(hood=hood, item=item):
                copy(own(item), hood, item, down).wait_send()
    for c in row_copies + col_copies:
        c.wait_send()


def exchange(rows, cols, vec, geo, coeff, share):
    chunks = vec.shape[0] // CHUNK
    vmem = pl.BlockSpec(memory_space=pltpu.VMEM)
    hbm = pl.BlockSpec(memory_space=pltpu.HBM)
    pool = lambda a: jax.ShapeDtypeStruct((9, *a.shape), a.dtype)
    dma = pltpu.SemaphoreType.DMA
    return pl.pallas_call(
        functools.partial(halo_kernel, rows, cols),
        out_shape=(pool(vec), pool(geo), pool(coeff), jax.ShapeDtypeStruct((cols, rows, *share.shape), F32)),
        in_specs=[vmem] * 4,
        out_specs=(hbm, hbm, hbm, vmem),
        scratch_shapes=[
            pltpu.VMEM((rows, *share.shape), F32),
            dma((9, chunks + 2)), dma((9, chunks + 2)),
            dma((rows,)), dma((rows,)), dma((cols,)), dma((cols,)), dma((4,)),
        ],
        compiler_params=pltpu.CompilerParams(
            collective_id=0, has_side_effects=True, vmem_limit_bytes=60 * 2**20
        ),
        name="halo",
    )(vec, geo, coeff, share)


GROUP = 8
RING = 32
STAGES = 4


def near_kernel(
    blocks, leaves, index, vec_pool, geo_pool,
    partial, mine, feats, vbuf, acc, stage, touched, vsem, gsem, ssem,
):
    width = vbuf.shape[2]
    count = 9 * leaves
    share = stage.shape[1]
    geo_copy = pltpu.make_async_copy(geo_pool, feats, gsem.at[0])
    geo_copy.start()

    def fetch(p, slot):
        hood, leaf = index[2, p], index[3, p]
        return pltpu.make_async_copy(
            vec_pool.at[hood, :, pl.ds(pl.multiple_of(leaf * width, width), width)], vbuf.at[slot], vsem.at[slot]
        )

    for p in range(RING):
        fetch(p, p).start()

    @pl.loop(0, count)
    def _(i):
        touched[i] = 0

    geo_copy.wait()

    def features(hood, leaf):
        return feats[hood, :, pl.ds(pl.multiple_of(leaf * width, width), width)].astype(F32)

    def power(p):
        tgt = features(index[0, p], index[1, p])
        src = features(index[2, p], index[3, p])
        left, right = left_rows(src).astype(BF16), right_rows(tgt).astype(BF16)
        return lax.dot_general(left, right, (((0,), (0,)), ((), ())), preferred_element_type=F32)

    @pl.loop(0, blocks // GROUP)
    def _(step):
        first = step * GROUP
        at = lax.rem(first, RING)
        for k in range(GROUP):
            fetch(first + k, at + k).wait()
        ahead = power(first)
        for k in range(GROUP):
            now = ahead
            if k + 1 < GROUP:
                ahead = power(first + k + 1)
            part = jnp.dot(vbuf[at + k], jnp.exp2(now).astype(BF16), preferred_element_type=F32)
            place = index[0, first + k] * leaves + index[1, first + k]
            seen = touched[place]
            touched[place] = 1
            acc[place] = jnp.where(seen > 0, acc[place], 0.0) + part

        @pl.when(first + RING < blocks)
        def _():
            for k in range(GROUP):
                fetch(first + RING + k, at + k).start()

    def settle(place):
        @pl.when(touched[place] == 0)
        def _():
            acc[place] = jnp.zeros(acc.shape[1:], F32)

    @pl.loop(0, leaves)
    def _(leaf):
        settle(4 * leaves + leaf)

    put_mine = pltpu.make_async_copy(acc.at[pl.ds(4 * leaves, leaves)], mine, gsem.at[0])
    put_mine.start()

    def put(hood, part):
        return pltpu.make_async_copy(
            stage.at[lax.rem(part, STAGES)], partial.at[hood, pl.ds(part * share, share)],
            ssem.at[lax.rem(part, STAGES)],
        )

    parts = leaves // share
    for hood in [h for h in range(9) if h != 4]:
        @pl.loop(0, parts)
        def _(part, hood=hood):
            if hood == 0:
                @pl.when(part >= STAGES)
                def _():
                    put(hood, part).wait()
            else:
                put(hood, part).wait()

            @pl.loop(0, share, unroll=4)
            def _(k):
                place = hood * leaves + part * share + k
                stage[lax.rem(part, STAGES), k] = jnp.where(touched[place] > 0, acc[place], 0.0).astype(BF16)

            put(hood, part).start()

    for slot in range(STAGES):
        put(0, slot).wait()
    put_mine.wait()


def near_blocks(index, vec_pool, geo_pool, leaves, width):
    blocks = index.shape[1]
    vecs = vec_pool.shape[1]
    share = leaves // STAGES
    hbm = pl.BlockSpec(memory_space=pl.ANY)
    dma = pltpu.SemaphoreType.DMA
    return pl.pallas_call(
        functools.partial(near_kernel, blocks, leaves),
        out_shape=(
            jax.ShapeDtypeStruct((9, leaves, vecs, width), BF16),
            jax.ShapeDtypeStruct((leaves, vecs, width), F32),
        ),
        in_specs=[pl.BlockSpec(memory_space=pltpu.SMEM), hbm, hbm],
        out_specs=(hbm, hbm),
        scratch_shapes=[
            pltpu.VMEM(geo_pool.shape, BF16),
            pltpu.VMEM((RING, vecs, width), BF16),
            pltpu.VMEM((9 * leaves, vecs, width), F32),
            pltpu.VMEM((STAGES, share, vecs, width), BF16),
            pltpu.SMEM((9 * leaves,), jnp.int32),
            dma((RING,)), dma((1,)), dma((STAGES,)),
        ],
        compiler_params=pltpu.CompilerParams(vmem_limit_bytes=58 * 2**20),
        name="near",
    )(index, vec_pool, geo_pool)


def left_rows(part):
    unit = lax.rem(lax.broadcasted_iota(jnp.int32, part.shape, 0), 4) == 3
    return jnp.concatenate([part, jnp.where(unit, 1.0, part)], axis=0)


def right_rows(part):
    row_id = lax.broadcasted_iota(jnp.int32, part.shape, 0)
    turned = jnp.concatenate([part[4:8], part[0:4]], axis=0)
    upper = jnp.where(lax.rem(row_id, 4) == 3, 1.0, jnp.where(row_id < 4, part, turned))
    return jnp.concatenate([upper, jnp.where(row_id < 3, turned, part)], axis=0)


def far_field(rank, far_index, top_index, own_top, coeff, skel, skel_rows, tops, turn, field):
    groups, vecs, lanes = field.shape
    members = lanes // rank
    partners = far_index.shape[1] // (groups * members)
    first_dim = (((0,), (0,)), ((), ()))
    lane = lax.broadcasted_iota(jnp.int32, (partners * rank, lanes), 1) // rank

    @pl.loop(0, 9)
    def _(hood):
        @pl.loop(0, groups)
        def _(q):
            part = skel[hood, :, pl.ds(pl.multiple_of(q * lanes, lanes), lanes)].astype(F32)
            turned = left_rows(part).T.astype(BF16)
            for member in range(members):
                skel_rows[(hood * groups + q) * members + member] = turned[member * rank : (member + 1) * rank]

    top = jnp.concatenate([tops[top_index[f]] for f in range(top_index.shape[0])], axis=0)
    total = None
    for k in range(3):
        gap = top[:, vecs + k : vecs + k + 1] - own_top[k : k + 1, :]
        total = gap * gap if total is None else total + gap * gap
    device_far = lax.dot_general(
        top[:, :vecs], jnp.exp(-0.5 * total), first_dim, precision=HIGH, preferred_element_type=F32
    )
    device_far = jnp.concatenate([device_far] * members, axis=1)
    square = lambda axis: lax.broadcasted_iota(jnp.int32, (lanes, lanes), axis) // rank
    same = square(0) == square(1)

    @pl.loop(0, groups)
    def _(q):
        right = right_rows(skel[4, :, pl.ds(pl.multiple_of(q * lanes, lanes), lanes)].astype(F32)).astype(BF16)
        back = turn[:, pl.ds(pl.multiple_of(q * lanes, lanes), lanes)].T
        back = jnp.where(same, jnp.concatenate([back] * members, axis=1), 0.0)
        total = jnp.dot(device_far, back, precision=HIGH, preferred_element_type=F32)
        for member in range(members):
            lefts, coeffs = [], []
            for f in range(partners):
                at = (q * members + member) * partners + f
                lefts.append(skel_rows[far_index[0, at]])
                both = coeff[far_index[1, at]]
                odd = jnp.full((rank, vecs), far_index[2, at], jnp.int32) > 0
                coeffs.append(jnp.where(odd, both[:, vecs:].astype(F32), both[:, :vecs].astype(F32)))
            left = jnp.concatenate(lefts, axis=0)
            picked = jnp.concatenate(coeffs, axis=0).astype(BF16)
            block = jnp.exp2(jnp.dot(left, right, preferred_element_type=F32))
            block = jnp.where(lane == member, block, 0.0)
            high = block.astype(BF16)
            low = (block - high.astype(F32)).astype(BF16)
            total += lax.dot_general(picked, high, first_dim, preferred_element_type=F32)
            total += lax.dot_general(picked, low, first_dim, preferred_element_type=F32)
        field[q] = total


def return_kernel(
    rows, cols, chunks, rank, far_index, top_index, own_top, partial, mine, coeff_pool, geo_pool, every, back, basis,
    out,
    from_rows, sums, from_cols, base, result, coeff, skel, skel_rows, tops, turn, base_rows, field,
    row_send, row_recv, col_send, col_recv, local, done,
):
    row, col = lax.axis_index("row"), lax.axis_index("col")
    has_row = (row > 0, row < rows - 1)
    has_col = (col > 0, col < cols - 1)
    leaves, vecs, width = base.shape
    share = leaves // chunks
    points = leaves * width
    pairs = [
        (partial.at[3], sums.at[0]), (partial.at[5], sums.at[1]), (coeff_pool, coeff),
        (geo_pool.at[:, :, pl.ds(points, leaves * rank)], skel), (every, tops), (back, turn),
        (basis, base_rows), (mine, base),
    ]
    loads = [pltpu.make_async_copy(src, dst, local.at[n]) for n, (src, dst) in enumerate(pairs)]
    for c in loads:
        c.start()
    barrier = pltpu.get_barrier_semaphore()
    row_dev = ((row - 1, col), (row + 1, col))
    col_dev = ((row, col - 1), (row, col + 1))
    peers = 0
    for has, dev in zip(has_row + has_col, row_dev + col_dev):
        peers = peers + has.astype(jnp.int32)

        @pl.when(has)
        def _(dev=dev):
            pl.semaphore_signal(barrier, inc=1, device_id=dev, device_id_type=MESH)
    pl.semaphore_wait(barrier, peers)

    def some(c):
        return pl.ds(c * share, share)

    def row_copy(side, place, c):
        hood = (0 if side == 0 else 6) + (0, 2, 1)[place]
        return remote(
            partial.at[hood, some(c)], from_rows.at[1 - side, place, some(c)],
            row_send.at[side, place, c], row_recv.at[1 - side, place, c], row_dev[side],
        )

    def col_copy(side, c):
        return remote(
            sums.at[side, some(c)], from_cols.at[1 - side, some(c)],
            col_send.at[side, c], col_recv.at[1 - side, c], col_dev[side],
        )

    def put(c):
        part = pl.ds(c * share * width, share * width)
        return pltpu.make_async_copy(result.at[:, part], out.at[:, part], done.at[c])

    wanted = has_col + (True,)
    plan = [(place, c) for c in range(chunks) for place in (0, 1)] + [(2, c) for c in range(chunks)]
    for place, c in plan:
        for side in (0, 1):
            @pl.when(has_row[side] & wanted[place])
            def _(side=side, place=place, c=c):
                row_copy(side, place, c).start()

    def fill(ref):
        @pl.loop(0, leaves)
        def _(i):
            ref[i] = jnp.zeros((vecs, width), BF16)

    for side in (0, 1):
        @pl.when(jnp.logical_not(has_row[side]))
        def _(side=side):
            for place in range(3):
                fill(from_rows.at[side, place])

        @pl.when(jnp.logical_not(has_col[side]))
        def _(side=side):
            fill(from_cols.at[side])

    for c in loads:
        c.wait()
    far_field(rank, far_index, top_index, own_top, coeff, skel, skel_rows, tops, turn, field)

    for c in range(chunks):
        for place in (0, 1):
            @pl.when(has_col[place])
            def _(place=place, c=c):
                for side in (0, 1):
                    @pl.when(has_row[side])
                    def _(side=side):
                        row_copy(1 - side, place, c).wait_recv()

                @pl.loop(c * share, (c + 1) * share)
                def _(i):
                    total = (
                        sums[place, i].astype(F32)
                        + from_rows[0, place, i].astype(F32)
                        + from_rows[1, place, i].astype(F32)
                    )
                    sums[place, i] = total.astype(BF16)

                col_copy(place, c).start()

    for c in range(chunks):
        for side in (0, 1):
            @pl.when(has_row[side])
            def _(side=side, c=c):
                row_copy(1 - side, 2, c).wait_recv()

            @pl.when(has_col[side])
            def _(side=side, c=c):
                col_copy(1 - side, c).wait_recv()

        group = 128 // rank
        lane = lax.broadcasted_iota(jnp.int32, (vecs, 128), 1) // rank

        @pl.loop(c * share, (c + 1) * share)
        def _(i):
            points_of = pl.ds(pl.multiple_of(i * width, width), width)
            weights = jnp.where(lane == lax.rem(i, group), field[i // group], 0.0).astype(BF16)
            spread = jnp.concatenate([base_rows[:, points_of]] * group, axis=0)
            result[:, points_of] = (
                jnp.dot(weights, spread, preferred_element_type=F32)
                + base[i]
                + from_rows[0, 2, i].astype(F32)
                + from_rows[1, 2, i].astype(F32)
                + from_cols[0, i].astype(F32)
                + from_cols[1, i].astype(F32)
            )

        put(c).start()

    for place, c in plan:
        for side in (0, 1):
            @pl.when(has_row[side] & wanted[place])
            def _(side=side, place=place, c=c):
                row_copy(side, place, c).wait_send()
    for c in range(chunks):
        for side in (0, 1):
            @pl.when(has_col[side])
            def _(side=side, c=c):
                col_copy(side, c).wait_send()
    for c in range(chunks):
        put(c).wait()


def give_back(rows, cols, far_index, top_index, own_top, partial, mine, coeff_pool, geo_pool, every, back, basis):
    leaves, vecs, width = mine.shape
    rank = basis.shape[0]
    chunks = math.gcd(leaves, 4)
    vmem, smem = pl.BlockSpec(memory_space=pltpu.VMEM), pl.BlockSpec(memory_space=pltpu.SMEM)
    hbm = pl.BlockSpec(memory_space=pltpu.HBM)
    dma = pltpu.SemaphoreType.DMA
    return pl.pallas_call(
        functools.partial(return_kernel, rows, cols, chunks, rank),
        out_shape=jax.ShapeDtypeStruct((vecs, leaves * width), F32),
        in_specs=[smem, smem, vmem] + [hbm] * 7,
        out_specs=hbm,
        scratch_shapes=[
            pltpu.VMEM((2, 3, leaves, vecs, width), BF16),
            pltpu.VMEM((2, leaves, vecs, width), BF16),
            pltpu.VMEM((2, leaves, vecs, width), BF16),
            pltpu.VMEM(mine.shape, F32),
            pltpu.VMEM((vecs, leaves * width), F32),
            pltpu.VMEM(coeff_pool.shape, BF16),
            pltpu.VMEM((9, 8, leaves * rank), BF16),
            pltpu.VMEM((9 * leaves, rank, 16), BF16),
            pltpu.VMEM(every.shape, F32),
            pltpu.VMEM(back.shape, F32),
            pltpu.VMEM(basis.shape, BF16),
            pltpu.VMEM((leaves * rank // 128, vecs, 128), F32),
            dma((2, 3, chunks)), dma((2, 3, chunks)), dma((2, chunks)), dma((2, chunks)), dma((8,)), dma((chunks,)),
        ],
        compiler_params=pltpu.CompilerParams(
            collective_id=1, has_side_effects=True, vmem_limit_bytes=56 * 2**20
        ),
        name="give_back",
    )(far_index, top_index, own_top, partial, mine, coeff_pool, geo_pool, every, back, basis)


def shards(
    coords, vectors, basis, transfer, leaf_skeleton, device_skeleton, near_pairs, far_leaves, far_devices
):
    row_count, col_count = lax.axis_size("row"), lax.axis_size("col")
    row_here, col_here = lax.axis_index("row"), lax.axis_index("col")
    rank_size, vec_count = basis.shape[0], vectors.shape[0]
    leaves = transfer.shape[1] // rank_size
    leaf_width = coords.shape[1] // leaves
    points = coords.shape[1]

    def hood_of(global_leaf):
        owner = global_leaf // leaves
        hood = (owner // col_count - row_here + 1) * 3 + (owner % col_count - col_here + 1)
        return hood, global_leaf % leaves

    geo = point_features(jnp.concatenate([coords, leaf_skeleton], axis=1))
    coeff = jnp.einsum(
        "vil,ril->irv",
        vectors.reshape(vec_count, leaves, leaf_width),
        basis.reshape(rank_size, leaves, leaf_width),
        preferred_element_type=F32,
    ).astype(BF16)
    transfer_mats = transfer.reshape(rank_size, leaves, rank_size)
    device_coeff = jnp.einsum("irv,ris->sv", coeff.astype(F32), transfer_mats, precision=HIGH)
    paired = coeff.reshape(leaves // 2, 2, rank_size, vec_count)
    paired = jnp.transpose(paired, (0, 2, 1, 3)).reshape(leaves // 2 * rank_size, 2 * vec_count)
    share = jnp.concatenate([device_coeff, device_skeleton.T], axis=1)
    share = jnp.pad(share, ((0, 0), (0, 128 - share.shape[1])))

    vec_pool, geo_pool, coeff_pool, every = exchange(row_count, col_count, vectors, geo, paired, share)

    t_hood, t_leaf = hood_of(near_pairs[0])
    s_hood, s_leaf = hood_of(near_pairs[1])
    index = jnp.stack([t_hood, t_leaf, s_hood, s_leaf])
    partial, mine = near_blocks(index, vec_pool, geo_pool, leaves, leaf_width)

    far_hood, far_leaf = hood_of(far_leaves.reshape(-1))
    far_place = far_hood * leaves + far_leaf
    far_index = jnp.stack([far_place, far_place // 2, far_place % 2])
    chosen = far_devices[0]
    top_index = chosen % col_count * row_count + chosen // col_count
    return give_back(
        row_count, col_count, far_index, top_index, device_skeleton,
        partial, mine, coeff_pool.reshape(-1, rank_size, 2 * vec_count), geo_pool,
        every.reshape(-1, *share.shape), transfer, basis,
    )


def solution(mesh):
    wide = P(None, ("row", "col"))
    tall = P(("row", "col"), None)
    return jax.shard_map(
        shards, mesh=mesh, in_specs=(wide,) * 7 + (tall,) * 2, out_specs=wide, check_vma=False
    )
```

```python
import functools
import math

import jax
import jax.numpy as jnp
from jax import lax
from jax.experimental import pallas as pl
from jax.experimental.pallas import tpu as pltpu
from jax.sharding import PartitionSpec as P

HIGH = lax.Precision.HIGHEST
F32 = jnp.float32
BF16 = jnp.bfloat16
MESH = pl.DeviceIdType.MESH
SCALE = math.sqrt(math.log2(math.e))
MIDDLE = 3.0
CHUNK = 16


def point_features(points):
    scaled = (points - MIDDLE) * SCALE
    high = lax.reduce_precision(scaled, 8, 7)
    low = lax.reduce_precision(scaled - high, 8, 7)
    whole = high + low
    norm = -0.5 * (whole[0:1] ** 2 + whole[1:2] ** 2 + whole[2:3] ** 2)
    norm_high = lax.reduce_precision(norm, 8, 7)
    return jnp.concatenate([high, norm_high, low, norm - norm_high], axis=0).astype(BF16)


def remote(src, dst, send, recv, device):
    return pltpu.make_async_remote_copy(
        src_ref=src, dst_ref=dst, send_sem=send, recv_sem=recv, device_id=device, device_id_type=MESH
    )


def halo_kernel(
    rows, cols, vec, geo, coeff, share,
    vec_pool, geo_pool, coeff_pool, every,
    row_share, send, recv, turn_send, row_send, row_recv, col_send, col_recv, local,
):
    row, col = lax.axis_index("row"), lax.axis_index("col")
    barrier = pltpu.get_barrier_semaphore()
    for d in range(1, rows):
        pl.semaphore_signal(barrier, inc=1, device_id=(lax.rem(row + d, rows), col), device_id_type=MESH)
    for d in range(1, cols):
        pl.semaphore_signal(barrier, inc=1, device_id=(row, lax.rem(col + d, cols)), device_id_type=MESH)
    pl.semaphore_wait(barrier, rows + cols - 2)

    chunks = vec.shape[0] // CHUNK
    items = chunks + 2
    first = [0, chunks, chunks + 1] + list(range(1, chunks))
    order = first[1:] + [0]
    even = lax.rem(row, 2) == 0

    def own(item):
        if item < chunks:
            return vec.at[pl.ds(item * CHUNK, CHUNK)]
        return geo if item == chunks else coeff

    def slot(hood, item):
        if item < chunks:
            return vec_pool.at[hood, pl.ds(item * CHUNK, CHUNK)]
        return (geo_pool if item == chunks else coeff_pool).at[hood]

    def copy(src, hood, item, device):
        return remote(src, slot(hood, item), send.at[hood, item], recv.at[hood, item], device)

    has_up, has_down = row > 0, row < rows - 1
    has_left, has_right = col > 0, col < cols - 1
    up, down, left, right = (row - 1, col), (row + 1, col), (row, col - 1), (row, col + 1)

    row_copies = []
    for d in range(1, rows):
        c = remote(share, row_share.at[row], row_send.at[d], row_recv.at[d], (lax.rem(row + d, rows), col))
        c.start()
        row_copies.append(c)
    keep_share = pltpu.make_async_copy(share, row_share.at[row], local.at[0])
    keep_share.start()
    keeps = [
        pltpu.make_async_copy(vec, vec_pool.at[4], local.at[1]),
        pltpu.make_async_copy(geo, geo_pool.at[4], local.at[2]),
        pltpu.make_async_copy(coeff, coeff_pool.at[4], local.at[3]),
    ]
    for k in keeps:
        k.start()

    direct = [(has_right, right, 3, order), (has_left, left, 5, order), (has_down, down, 1, first), (has_up, up, 7, first)]
    half = lax.rem(row, 2)
    own_half = row_share.at[pl.ds(half * (rows // 2), rows // 2)]
    col_copies = []
    for n in range(items):
        for has, device, hood, sequence in direct:
            item = sequence[n]

            @pl.when(has)
            def _(device=device, hood=hood, item=item):
                copy(own(item), hood, item, device).start()

        if n == 0:
            keep_share.wait()
            for c in row_copies:
                c.wait_recv()
            for d in range(1, cols):
                c = remote(
                    own_half, every.at[half, col], col_send.at[d], col_recv.at[d], (row, lax.rem(col + d, cols))
                )
                c.start()
                col_copies.append(c)
            keep_row = pltpu.make_async_copy(own_half, every.at[half, col], local.at[0])
            keep_row.start()

    outward = [(1, has_up & even, 0, 2), (7, has_down & jnp.logical_not(even), 6, 8)]

    def turned(hood, target, device):
        return remote(slot(hood, 0), slot(target, 0), turn_send.at[target], recv.at[target, 0], device)

    for hood, has, to_right, to_left in outward:
        @pl.when(has)
        def _(hood=hood, to_right=to_right, to_left=to_left):
            copy(own(0), hood, 0, down).wait_recv()

            @pl.when(has_right)
            def _():
                turned(hood, to_right, right).start()

            @pl.when(has_left)
            def _():
                turned(hood, to_left, left).start()

    passed = [(3, has_left, 0, 6), (5, has_right, 2, 8)]
    for item in order:
        for hood, has, to_down, to_up in passed:
            @pl.when(has)
            def _(hood=hood, item=item, to_down=to_down, to_up=to_up):
                copy(own(item), hood, item, down).wait_recv()

                @pl.when(has_down & even if item == 0 else has_down)
                def _():
                    copy(slot(hood, item), to_down, item, down).start()

                @pl.when(has_up & jnp.logical_not(even) if item == 0 else has_up)
                def _():
                    copy(slot(hood, item), to_up, item, up).start()

    keep_row.wait()
    for c in col_copies:
        c.wait_recv()
    swap = remote(every.at[half], every.at[half], turn_send.at[1], turn_send.at[3], (row + 1 - 2 * half, col))
    swap.start()
    for k in keeps:
        k.wait()
    odd = jnp.logical_not(even)
    for item in order:
        for has, hood in [
            (has_up & odd if item == 0 else has_up, 1), (has_down & even if item == 0 else has_down, 7),
            (has_up & has_left, 0), (has_up & has_right, 2),
            (has_down & has_left, 6), (has_down & has_right, 8),
        ]:
            @pl.when(has)
            def _(hood=hood, item=item):
                copy(own(item), hood, item, down).wait_recv()
    for item in order:
        to_down, to_up = (has_down & even, has_up & odd) if item == 0 else (has_down, has_up)
        for has, hood in [
            (has_right, 3), (has_left, 5), (has_down, 1), (has_up, 7),
            (to_down & has_left, 0), (to_up & has_left, 6),
            (to_down & has_right, 2), (to_up & has_right, 8),
        ]:
            @pl.when(has)
            def _(hood=hood, item=item):
                copy(own(item), hood, item, down).wait_send()
    for hood, has, to_right, to_left in outward:
        for side, target, device in ((has_right, to_right, right), (has_left, to_left, left)):
            @pl.when(has & side)
            def _(hood=hood, target=target, device=device):
                turned(hood, target, device).wait_send()
    for c in row_copies + col_copies:
        c.wait_send()
    swap.wait()


def exchange(rows, cols, vec, geo, coeff, share):
    chunks = vec.shape[0] // CHUNK
    vmem = pl.BlockSpec(memory_space=pltpu.VMEM)
    hbm = pl.BlockSpec(memory_space=pltpu.HBM)
    pool = lambda a: jax.ShapeDtypeStruct((9, *a.shape), a.dtype)
    dma = pltpu.SemaphoreType.DMA
    return pl.pallas_call(
        functools.partial(halo_kernel, rows, cols),
        out_shape=(pool(vec), pool(geo), pool(coeff), jax.ShapeDtypeStruct((2, cols, rows // 2, *share.shape), BF16)),
        in_specs=[vmem] * 4,
        out_specs=(hbm, hbm, hbm, vmem),
        scratch_shapes=[
            pltpu.VMEM((rows, *share.shape), BF16),
            dma((9, chunks + 2)), dma((9, chunks + 2)), dma((9,)),
            dma((rows,)), dma((rows,)), dma((cols,)), dma((cols,)), dma((4,)),
        ],
        compiler_params=pltpu.CompilerParams(
            collective_id=0, has_side_effects=True, vmem_limit_bytes=60 * 2**20
        ),
        name="halo",
    )(vec, geo, coeff, share)


GROUP = 32
AHEAD = 4
RING = 64
STAGES = 4


def near_kernel(
    blocks, leaves, index, vec_pool, geo_pool,
    partial, mine, feats, vbuf, acc, stage, touched, vsem, gsem, ssem,
):
    width = vbuf.shape[2]
    count = 9 * leaves
    share = stage.shape[1]
    geo_copy = pltpu.make_async_copy(geo_pool, feats, gsem.at[0])
    geo_copy.start()

    def fetch(p, slot):
        hood, leaf = index[2, p], index[3, p]
        return pltpu.make_async_copy(
            vec_pool.at[hood, :, pl.ds(pl.multiple_of(leaf * width, width), width)], vbuf.at[slot], vsem.at[slot]
        )

    for p in range(RING):
        fetch(p, p).start()

    @pl.loop(0, count)
    def _(i):
        touched[i] = 0

    geo_copy.wait()

    def features(hood, leaf):
        return feats[hood, :, pl.ds(pl.multiple_of(leaf * width, width), width)].astype(F32)

    def power(p):
        tgt = features(index[0, p], index[1, p])
        src = features(index[2, p], index[3, p])
        left, right = left_rows(src).astype(BF16), right_rows(tgt).astype(BF16)
        return lax.dot_general(left, right, (((0,), (0,)), ((), ())), preferred_element_type=F32)

    @pl.loop(0, blocks // GROUP)
    def _(step):
        first = step * GROUP
        at = lax.rem(first, RING)
        for k in range(GROUP):
            fetch(first + k, at + k).wait()
        ahead = [power(first + k) for k in range(AHEAD)]
        for k in range(GROUP):
            now = ahead.pop(0)
            if k + AHEAD < GROUP:
                ahead.append(power(first + k + AHEAD))
            part = jnp.dot(vbuf[at + k], jnp.exp2(now).astype(BF16), preferred_element_type=F32)
            place = index[0, first + k] * leaves + index[1, first + k]
            seen = touched[place]
            touched[place] = 1
            acc[place] = jnp.where(seen > 0, acc[place], 0.0) + part

        @pl.when(first + RING < blocks)
        def _():
            for k in range(GROUP):
                fetch(first + RING + k, at + k).start()

    def settle(place):
        @pl.when(touched[place] == 0)
        def _():
            acc[place] = jnp.zeros(acc.shape[1:], F32)

    @pl.loop(0, leaves)
    def _(leaf):
        settle(4 * leaves + leaf)

    put_mine = pltpu.make_async_copy(acc.at[pl.ds(4 * leaves, leaves)], mine, gsem.at[0])
    put_mine.start()

    def put(hood, part):
        return pltpu.make_async_copy(
            stage.at[lax.rem(part, STAGES)], partial.at[hood, pl.ds(part * share, share)],
            ssem.at[lax.rem(part, STAGES)],
        )

    parts = leaves // share
    for hood in [h for h in range(9) if h != 4]:
        @pl.loop(0, parts)
        def _(part, hood=hood):
            if hood == 0:
                @pl.when(part >= STAGES)
                def _():
                    put(hood, part).wait()
            else:
                put(hood, part).wait()

            @pl.loop(0, share, unroll=4)
            def _(k):
                place = hood * leaves + part * share + k
                stage[lax.rem(part, STAGES), k] = jnp.where(touched[place] > 0, acc[place], 0.0).astype(BF16)

            put(hood, part).start()

    for slot in range(STAGES):
        put(0, slot).wait()
    put_mine.wait()


def near_blocks(index, vec_pool, geo_pool, leaves, width):
    blocks = index.shape[1]
    vecs = vec_pool.shape[1]
    share = leaves // STAGES
    hbm = pl.BlockSpec(memory_space=pl.ANY)
    dma = pltpu.SemaphoreType.DMA
    return pl.pallas_call(
        functools.partial(near_kernel, blocks, leaves),
        out_shape=(
            jax.ShapeDtypeStruct((9, leaves, vecs, width), BF16),
            jax.ShapeDtypeStruct((leaves, vecs, width), F32),
        ),
        in_specs=[pl.BlockSpec(memory_space=pltpu.SMEM), hbm, hbm],
        out_specs=(hbm, hbm),
        scratch_shapes=[
            pltpu.VMEM(geo_pool.shape, BF16),
            pltpu.VMEM((RING, vecs, width), BF16),
            pltpu.VMEM((9 * leaves, vecs, width), F32),
            pltpu.VMEM((STAGES, share, vecs, width), BF16),
            pltpu.SMEM((9 * leaves,), jnp.int32),
            dma((RING,)), dma((1,)), dma((STAGES,)),
        ],
        compiler_params=pltpu.CompilerParams(vmem_limit_bytes=58 * 2**20),
        name="near",
    )(index, vec_pool, geo_pool)


def left_rows(part):
    unit = lax.rem(lax.broadcasted_iota(jnp.int32, part.shape, 0), 4) == 3
    return jnp.concatenate([part, jnp.where(unit, 1.0, part)], axis=0)


def right_rows(part):
    row_id = lax.broadcasted_iota(jnp.int32, part.shape, 0)
    turned = jnp.concatenate([part[4:8], part[0:4]], axis=0)
    upper = jnp.where(lax.rem(row_id, 4) == 3, 1.0, jnp.where(row_id < 4, part, turned))
    return jnp.concatenate([upper, jnp.where(row_id < 3, turned, part)], axis=0)


def far_field(rank, far_index, top_index, own_top, coeff, skel, skel_rows, tops, turn, field, chunks):
    groups, vecs, lanes = field.shape
    members = lanes // rank
    partners = far_index.shape[1] // (groups * members)
    first_dim = (((0,), (0,)), ((), ()))
    lane = lax.broadcasted_iota(jnp.int32, (partners * rank, lanes), 1) // rank

    @pl.loop(0, 9)
    def _(hood):
        @pl.loop(0, groups)
        def _(q):
            part = skel[hood, :, pl.ds(pl.multiple_of(q * lanes, lanes), lanes)].astype(F32)
            turned = left_rows(part).T.astype(BF16)
            for member in range(members):
                skel_rows[(hood * groups + q) * members + member] = turned[member * rank : (member + 1) * rank]

    chosen = [tops[top_index[f]].astype(F32) for f in range(top_index.shape[0])]
    top = jnp.concatenate([c[:rank, :vecs] + c[:rank, vecs:] for c in chosen], axis=0)
    parts = jnp.concatenate([c[rank:].T[:rank] for c in chosen], axis=0)
    spots = parts[:, 0:3] + parts[:, 3:6] + parts[:, 6:9]
    total = None
    for k in range(3):
        gap = spots[:, k : k + 1] - own_top[k : k + 1, :]
        total = gap * gap if total is None else total + gap * gap
    device_far = lax.dot_general(
        top, jnp.exp(-0.5 * total), first_dim, precision=HIGH, preferred_element_type=F32
    )
    device_far = jnp.concatenate([device_far] * members, axis=1)
    square = lambda axis: lax.broadcasted_iota(jnp.int32, (lanes, lanes), axis) // rank
    same = square(0) == square(1)

    def part(c):
        @pl.loop(c * groups // chunks, (c + 1) * groups // chunks)
        def _(q):
            right = right_rows(skel[4, :, pl.ds(pl.multiple_of(q * lanes, lanes), lanes)].astype(F32)).astype(BF16)
            back = turn[:, pl.ds(pl.multiple_of(q * lanes, lanes), lanes)].T
            back = jnp.where(same, jnp.concatenate([back] * members, axis=1), 0.0)
            total = jnp.dot(device_far, back, precision=HIGH, preferred_element_type=F32)
            for member in range(members):
                lefts, coeffs = [], []
                for f in range(partners):
                    at = (q * members + member) * partners + f
                    lefts.append(skel_rows[far_index[0, at]])
                    both = coeff[far_index[1, at]]
                    odd = jnp.full((rank, vecs), far_index[2, at], jnp.int32) > 0
                    coeffs.append(jnp.where(odd, both[:, vecs:].astype(F32), both[:, :vecs].astype(F32)))
                left = jnp.concatenate(lefts, axis=0)
                picked = jnp.concatenate(coeffs, axis=0).astype(BF16)
                block = jnp.exp2(jnp.dot(left, right, preferred_element_type=F32))
                block = jnp.where(lane == member, block, 0.0)
                high = block.astype(BF16)
                low = (block - high.astype(F32)).astype(BF16)
                total += lax.dot_general(picked, high, first_dim, preferred_element_type=F32)
                total += lax.dot_general(picked, low, first_dim, preferred_element_type=F32)
            field[q] = total

    return part


def return_kernel(
    rows, cols, chunks, rank, far_index, top_index, own_top, partial, mine, coeff_pool, geo_pool, every, back, basis,
    out,
    from_rows, sums, from_cols, base, result, coeff, skel, skel_rows, tops, turn, base_rows, field, crossed, passing,
    row_send, row_recv, col_send, col_recv, cross_send, cross_recv, local, done,
):
    row, col = lax.axis_index("row"), lax.axis_index("col")
    has_row = (row > 0, row < rows - 1)
    has_col = (col > 0, col < cols - 1)
    leaves, vecs, width = base.shape
    share = leaves // chunks
    points = leaves * width
    parity = lax.rem(row, 2)
    leaving = (has_row[0] & (parity == 0), has_row[1] & (parity == 1))

    def side_of(place):
        return parity * 6 + place

    pairs = [
        (partial.at[3], sums.at[0]), (partial.at[5], sums.at[1]), (coeff_pool, coeff),
        (geo_pool.at[:, :, pl.ds(points, leaves * rank)], skel), (every, tops), (back, turn),
        (basis, base_rows), (mine, base), (partial.at[side_of(1), pl.ds(0, share)], passing),
    ]
    loads = [pltpu.make_async_copy(src, dst, local.at[n]) for n, (src, dst) in enumerate(pairs)]
    for c in loads:
        c.start()
    barrier = pltpu.get_barrier_semaphore()
    row_dev = ((row - 1, col), (row + 1, col))
    col_dev = ((row, col - 1), (row, col + 1))
    peers = 0
    for has, dev in zip(has_row + has_col, row_dev + col_dev):
        peers = peers + has.astype(jnp.int32)

        @pl.when(has)
        def _(dev=dev):
            pl.semaphore_signal(barrier, inc=1, device_id=dev, device_id_type=MESH)
    pl.semaphore_wait(barrier, peers)

    def some(c):
        return pl.ds(c * share, share)

    def row_copy(side, place, c, src=None):
        hood = (0 if side == 0 else 6) + (0, 2, 1)[place]
        return remote(
            partial.at[hood, some(c)] if src is None else src, from_rows.at[1 - side, place, some(c)],
            row_send.at[side, place, c], row_recv.at[1 - side, place, c], row_dev[side],
        )

    def col_copy(side, c):
        return remote(
            sums.at[side, some(c)], from_cols.at[1 - side, some(c)],
            col_send.at[side, c], col_recv.at[1 - side, c], col_dev[side],
        )

    def cross_copy(side):
        return remote(
            partial.at[side_of(2 * side), pl.ds(0, share)], crossed.at[1 - side],
            cross_send.at[side], cross_recv.at[1 - side], col_dev[side],
        )

    def put(c):
        part = pl.ds(c * share * width, share * width)
        return pltpu.make_async_copy(result.at[:, part], out.at[:, part], done.at[c])

    crossing = leaving[0] | leaving[1]
    for side in (0, 1):
        @pl.when(crossing & has_col[side])
        def _(side=side):
            cross_copy(side).start()

    def sent(side, place, c):
        if c > 0:
            return has_row[side] & (has_col[place] if place < 2 else True)
        stays = has_row[side] & (parity != side)
        return stays & has_col[place] if place < 2 else stays

    later = list(range(1, chunks))
    plan = [(place, 0) for place in (0, 1, 2)] + [(place, c) for c in later for place in (0, 1)]
    plan += [(2, c) for c in later]
    for place, c in plan:
        for side in (0, 1):
            @pl.when(sent(side, place, c))
            def _(side=side, place=place, c=c):
                row_copy(side, place, c).start()

    def fill(ref):
        @pl.loop(0, ref.shape[0])
        def _(i):
            ref[i] = jnp.zeros((vecs, width), BF16)

    for side in (0, 1):
        @pl.when(jnp.logical_not(has_row[side]))
        def _(side=side):
            for place in range(3):
                fill(from_rows.at[side, place])

        @pl.when(leaving[side])
        def _(side=side):
            for place in range(2):
                fill(from_rows.at[side, place, pl.ds(0, share)])

        @pl.when(jnp.logical_not(has_col[side]))
        def _(side=side):
            fill(from_cols.at[side])
            fill(crossed.at[side])

    for c in loads:
        c.wait()
    parts = far_field(rank, far_index, top_index, own_top, coeff, skel, skel_rows, tops, turn, field, chunks)

    @pl.when(crossing)
    def _():
        for side in (0, 1):
            @pl.when(has_col[side])
            def _(side=side):
                cross_copy(1 - side).wait_recv()

        @pl.loop(0, share)
        def _(i):
            total = passing[i].astype(F32) + crossed[0, i].astype(F32) + crossed[1, i].astype(F32)
            passing[i] = total.astype(BF16)

        for side in (0, 1):
            @pl.when(leaving[side])
            def _(side=side):
                row_copy(side, 2, 0, passing).start()

    for c in range(chunks):
        for place in (0, 1):
            @pl.when(has_col[place])
            def _(place=place, c=c):
                for side in (0, 1):
                    @pl.when(has_row[side] if c > 0 else has_row[side] & (parity != side))
                    def _(side=side):
                        row_copy(1 - side, place, c).wait_recv()

                @pl.loop(c * share, (c + 1) * share)
                def _(i):
                    total = (
                        sums[place, i].astype(F32)
                        + from_rows[0, place, i].astype(F32)
                        + from_rows[1, place, i].astype(F32)
                    )
                    sums[place, i] = total.astype(BF16)

                col_copy(place, c).start()

        parts(c)

    for c in range(chunks):
        for side in (0, 1):
            @pl.when(has_row[side])
            def _(side=side, c=c):
                row_copy(1 - side, 2, c).wait_recv()

            @pl.when(has_col[side])
            def _(side=side, c=c):
                col_copy(1 - side, c).wait_recv()

        group = 128 // rank
        lane = lax.broadcasted_iota(jnp.int32, (vecs, 128), 1) // rank

        @pl.loop(c * share, (c + 1) * share)
        def _(i):
            points_of = pl.ds(pl.multiple_of(i * width, width), width)
            weights = jnp.where(lane == lax.rem(i, group), field[i // group], 0.0).astype(BF16)
            spread = jnp.concatenate([base_rows[:, points_of]] * group, axis=0)
            result[:, points_of] = (
                jnp.dot(weights, spread, preferred_element_type=F32)
                + base[i]
                + from_rows[0, 2, i].astype(F32)
                + from_rows[1, 2, i].astype(F32)
                + from_cols[0, i].astype(F32)
                + from_cols[1, i].astype(F32)
            )

        put(c).start()

    for place, c in plan:
        for side in (0, 1):
            @pl.when(sent(side, place, c))
            def _(side=side, place=place, c=c):
                row_copy(side, place, c).wait_send()
    for side in (0, 1):
        @pl.when(leaving[side])
        def _(side=side):
            row_copy(side, 2, 0, passing).wait_send()

        @pl.when(crossing & has_col[side])
        def _(side=side):
            cross_copy(side).wait_send()
    for c in range(chunks):
        for side in (0, 1):
            @pl.when(has_col[side])
            def _(side=side, c=c):
                col_copy(side, c).wait_send()
    for c in range(chunks):
        put(c).wait()


def give_back(rows, cols, far_index, top_index, own_top, partial, mine, coeff_pool, geo_pool, every, back, basis):
    leaves, vecs, width = mine.shape
    rank = basis.shape[0]
    chunks = math.gcd(leaves, 4)
    vmem, smem = pl.BlockSpec(memory_space=pltpu.VMEM), pl.BlockSpec(memory_space=pltpu.SMEM)
    hbm = pl.BlockSpec(memory_space=pltpu.HBM)
    dma = pltpu.SemaphoreType.DMA
    return pl.pallas_call(
        functools.partial(return_kernel, rows, cols, chunks, rank),
        out_shape=jax.ShapeDtypeStruct((vecs, leaves * width), F32),
        in_specs=[smem, smem, vmem] + [hbm] * 7,
        out_specs=hbm,
        scratch_shapes=[
            pltpu.VMEM((2, 3, leaves, vecs, width), BF16),
            pltpu.VMEM((2, leaves, vecs, width), BF16),
            pltpu.VMEM((2, leaves, vecs, width), BF16),
            pltpu.VMEM(mine.shape, F32),
            pltpu.VMEM((vecs, leaves * width), F32),
            pltpu.VMEM(coeff_pool.shape, BF16),
            pltpu.VMEM((9, 8, leaves * rank), BF16),
            pltpu.VMEM((9 * leaves, rank, 16), BF16),
            pltpu.VMEM(every.shape, BF16),
            pltpu.VMEM(back.shape, F32),
            pltpu.VMEM(basis.shape, BF16),
            pltpu.VMEM((leaves * rank // 128, vecs, 128), F32),
            pltpu.VMEM((2, leaves // chunks, vecs, width), BF16),
            pltpu.VMEM((leaves // chunks, vecs, width), BF16),
            dma((2, 3, chunks)), dma((2, 3, chunks)), dma((2, chunks)), dma((2, chunks)), dma((2,)), dma((2,)), dma((9,)), dma((chunks,)),
        ],
        compiler_params=pltpu.CompilerParams(
            collective_id=1, has_side_effects=True, vmem_limit_bytes=56 * 2**20
        ),
        name="give_back",
    )(far_index, top_index, own_top, partial, mine, coeff_pool, geo_pool, every, back, basis)


def shards(
    coords, vectors, basis, transfer, leaf_skeleton, device_skeleton, near_pairs, far_leaves, far_devices
):
    row_count, col_count = lax.axis_size("row"), lax.axis_size("col")
    row_here, col_here = lax.axis_index("row"), lax.axis_index("col")
    rank_size, vec_count = basis.shape[0], vectors.shape[0]
    leaves = transfer.shape[1] // rank_size
    leaf_width = coords.shape[1] // leaves
    points = coords.shape[1]

    def hood_of(global_leaf):
        owner = global_leaf // leaves
        hood = (owner // col_count - row_here + 1) * 3 + (owner % col_count - col_here + 1)
        return hood, global_leaf % leaves

    geo = point_features(jnp.concatenate([coords, leaf_skeleton], axis=1))
    coeff = jnp.einsum(
        "vil,ril->irv",
        vectors.reshape(vec_count, leaves, leaf_width),
        basis.reshape(rank_size, leaves, leaf_width),
        preferred_element_type=F32,
    ).astype(BF16)
    transfer_mats = transfer.reshape(rank_size, leaves, rank_size)
    device_coeff = jnp.einsum("irv,ris->sv", coeff.astype(F32), transfer_mats, precision=HIGH)
    paired = coeff.reshape(leaves // 2, 2, rank_size, vec_count)
    paired = jnp.transpose(paired, (0, 2, 1, 3)).reshape(leaves // 2 * rank_size, 2 * vec_count)
    coeff_high = lax.reduce_precision(device_coeff, 8, 7)
    parts, rest = [], device_skeleton
    for _ in range(3):
        parts.append(lax.reduce_precision(rest, 8, 7))
        rest = rest - parts[-1]
    spots = jnp.pad(jnp.concatenate(parts, axis=0), ((0, 7), (0, 2 * vec_count - rank_size)))
    share = jnp.concatenate(
        [jnp.concatenate([coeff_high, device_coeff - coeff_high], axis=1), spots], axis=0
    ).astype(BF16)

    vec_pool, geo_pool, coeff_pool, every = exchange(row_count, col_count, vectors, geo, paired, share)

    t_hood, t_leaf = hood_of(near_pairs[0])
    s_hood, s_leaf = hood_of(near_pairs[1])
    index = jnp.stack([t_hood, t_leaf, s_hood, s_leaf])
    partial, mine = near_blocks(index, vec_pool, geo_pool, leaves, leaf_width)

    far_hood, far_leaf = hood_of(far_leaves.reshape(-1))
    far_place = far_hood * leaves + far_leaf
    far_index = jnp.stack([far_place, far_place // 2, far_place % 2])
    chosen = far_devices[0]
    rows_half = row_count // 2
    top_row, top_col = chosen // col_count, chosen % col_count
    top_index = (top_row // rows_half * col_count + top_col) * rows_half + top_row % rows_half
    return give_back(
        row_count, col_count, far_index, top_index, device_skeleton,
        partial, mine, coeff_pool.reshape(-1, rank_size, 2 * vec_count), geo_pool,
        every.reshape(-1, *share.shape), transfer, basis,
    )


def solution(mesh):
    wide = P(None, ("row", "col"))
    tall = P(("row", "col"), None)
    return jax.shard_map(
        shards, mesh=mesh, in_specs=(wide,) * 7 + (tall,) * 2, out_specs=wide, check_vma=False
    )
```

```python
import functools
import math

import jax
import jax.numpy as jnp
from jax import lax
from jax.experimental import pallas as pl
from jax.experimental.pallas import tpu as pltpu
from jax.sharding import PartitionSpec as P

HIGH = lax.Precision.HIGHEST
F32 = jnp.float32
BF16 = jnp.bfloat16
MESH = pl.DeviceIdType.MESH
SCALE = math.sqrt(math.log2(math.e))
MIDDLE = 3.0
CHUNK = 16


def rounded(x):
    return x.astype(BF16).astype(F32)


def point_features(points):
    scaled = (points - MIDDLE) * SCALE
    high = rounded(scaled)
    low = rounded(scaled - high)
    whole = high + low
    norm = -0.5 * (whole[0:1] * whole[0:1] + whole[1:2] * whole[1:2] + whole[2:3] * whole[2:3])
    norm_high = rounded(norm)
    return jnp.concatenate([high, norm_high, low, norm - norm_high], axis=0).astype(BF16)


STRIP = 1024


def own_terms(vec, coords, skeleton, basis, transfer, device_skeleton, geo, coeff, share):
    vecs, points = vec.shape
    rank = basis.shape[0]
    leaves = transfer.shape[1] // rank
    width = points // leaves
    members = 128 // rank

    def group(q, total):
        back = transfer[:, pl.ds(pl.multiple_of(q * 128, 128), 128)].T
        blocks = []
        for m in range(members):
            lanes = pl.ds(pl.multiple_of((q * members + m) * width, width), width)
            block = lax.dot_general(
                basis[:, lanes], vec[:, lanes], (((1,), (1,)), ((), ())), preferred_element_type=F32
            )
            blocks.append(rounded(block))
        wide = jnp.concatenate([back[m * rank : (m + 1) * rank] for m in range(members)], axis=1)
        total += jnp.dot(wide, jnp.concatenate(blocks, axis=0), precision=HIGH, preferred_element_type=F32)
        for k in range(members // 2):
            rows_of = pl.ds(pl.multiple_of((q * (members // 2) + k) * rank, rank), rank)
            coeff[rows_of, :] = jnp.concatenate(blocks[2 * k : 2 * k + 2], axis=1).astype(BF16)
        return total

    device_coeff = lax.fori_loop(0, leaves // members, group, jnp.zeros((rank, vecs), F32))
    high = rounded(device_coeff)
    share[0:rank, :] = jnp.concatenate([high, device_coeff - high], axis=1).astype(BF16)
    parts, rest = [], device_skeleton[...]
    for _ in range(3):
        parts.append(rounded(rest))
        rest = rest - parts[-1]
    parts.append(jnp.zeros((7, rank), F32))
    share[rank:, :] = jnp.concatenate([jnp.concatenate(parts, axis=0)] * members, axis=1).astype(BF16)

    for source, start in ((coords, 0), (skeleton, points)):
        @pl.loop(0, source.shape[1] // STRIP)
        def _(i, source=source, start=start):
            at = pl.multiple_of(i * STRIP, STRIP)
            geo[:, pl.ds(start + at, STRIP)] = point_features(source[:, pl.ds(at, STRIP)])


def remote(src, dst, send, recv, device):
    return pltpu.make_async_remote_copy(
        src_ref=src, dst_ref=dst, send_sem=send, recv_sem=recv, device_id=device, device_id_type=MESH
    )


def halo_kernel(
    rows, cols, vec, coords, skeleton, basis, transfer, device_skeleton,
    vec_pool, geo_pool, coeff_pool, every,
    geo, coeff, share, row_share, send, recv, turn_send, row_send, row_recv, col_send, col_recv, local,
):
    row, col = lax.axis_index("row"), lax.axis_index("col")
    barrier = pltpu.get_barrier_semaphore()
    for d in range(1, rows):
        pl.semaphore_signal(barrier, inc=1, device_id=(lax.rem(row + d, rows), col), device_id_type=MESH)
    for d in range(1, cols):
        pl.semaphore_signal(barrier, inc=1, device_id=(row, lax.rem(col + d, cols)), device_id_type=MESH)
    pl.semaphore_wait(barrier, rows + cols - 2)

    chunks = vec.shape[0] // CHUNK
    items = chunks + 2
    early = list(range(chunks))
    order = list(range(1, chunks)) + [0, chunks, chunks + 1]
    even = lax.rem(row, 2) == 0

    def own(item):
        if item < chunks:
            return vec.at[pl.ds(item * CHUNK, CHUNK)]
        return geo if item == chunks else coeff

    def slot(hood, item):
        if item < chunks:
            return vec_pool.at[hood, pl.ds(item * CHUNK, CHUNK)]
        return (geo_pool if item == chunks else coeff_pool).at[hood]

    def copy(src, hood, item, device):
        return remote(src, slot(hood, item), send.at[hood, item], recv.at[hood, item], device)

    has_up, has_down = row > 0, row < rows - 1
    has_left, has_right = col > 0, col < cols - 1
    up, down, left, right = (row - 1, col), (row + 1, col), (row, col - 1), (row, col + 1)

    def give(has, device, hood, item):
        @pl.when(has)
        def _():
            copy(own(item), hood, item, device).start()

    along_row = [(has_down, down, 1), (has_up, up, 7)]
    along_col = [(has_right, right, 3), (has_left, left, 5)]
    for item in early:
        for direct in along_row:
            give(*direct, item)
    for item in order[:chunks]:
        for direct in along_col:
            give(*direct, item)
    keeps = [pltpu.make_async_copy(vec, vec_pool.at[4], local.at[1])]
    keeps[0].start()

    own_terms(vec, coords, skeleton, basis, transfer, device_skeleton, geo, coeff, share)

    row_copies = []
    for d in range(1, rows):
        c = remote(share, row_share.at[row], row_send.at[d], row_recv.at[d], (lax.rem(row + d, rows), col))
        c.start()
        row_copies.append(c)
    keep_share = pltpu.make_async_copy(share, row_share.at[row], local.at[0])
    keep_share.start()
    for n, (mine, pool) in enumerate(((geo, geo_pool), (coeff, coeff_pool))):
        keeps.append(pltpu.make_async_copy(mine, pool.at[4], local.at[2 + n]))
        keeps[-1].start()
    for item in (chunks, chunks + 1):
        for direct in along_row:
            give(*direct, item)

    half = lax.rem(row, 2)
    own_half = row_share.at[pl.ds(half * (rows // 2), rows // 2)]
    col_copies = []
    keep_share.wait()
    for c in row_copies:
        c.wait_recv()
    for d in range(1, cols):
        c = remote(own_half, every.at[half, col], col_send.at[d], col_recv.at[d], (row, lax.rem(col + d, cols)))
        c.start()
        col_copies.append(c)
    keep_row = pltpu.make_async_copy(own_half, every.at[half, col], local.at[0])
    keep_row.start()
    for item in order[chunks:]:
        for direct in along_col:
            give(*direct, item)

    outward = [(1, has_up & even, 0, 2), (7, has_down & jnp.logical_not(even), 6, 8)]

    def turned(hood, target, device):
        return remote(slot(hood, 0), slot(target, 0), turn_send.at[target], recv.at[target, 0], device)

    for hood, has, to_right, to_left in outward:
        @pl.when(has)
        def _(hood=hood, to_right=to_right, to_left=to_left):
            copy(own(0), hood, 0, down).wait_recv()

            @pl.when(has_right)
            def _():
                turned(hood, to_right, right).start()

            @pl.when(has_left)
            def _():
                turned(hood, to_left, left).start()

    passed = [(3, has_left, 0, 6), (5, has_right, 2, 8)]
    for item in order:
        for hood, has, to_down, to_up in passed:
            @pl.when(has)
            def _(hood=hood, item=item, to_down=to_down, to_up=to_up):
                copy(own(item), hood, item, down).wait_recv()

                @pl.when(has_down & even if item == 0 else has_down)
                def _():
                    copy(slot(hood, item), to_down, item, down).start()

                @pl.when(has_up & jnp.logical_not(even) if item == 0 else has_up)
                def _():
                    copy(slot(hood, item), to_up, item, up).start()

    keep_row.wait()
    for c in col_copies:
        c.wait_recv()
    swap = remote(every.at[half], every.at[half], turn_send.at[1], turn_send.at[3], (row + 1 - 2 * half, col))
    swap.start()
    for k in keeps:
        k.wait()
    odd = jnp.logical_not(even)
    for item in order:
        for has, hood in [
            (has_up & odd if item == 0 else has_up, 1), (has_down & even if item == 0 else has_down, 7),
            (has_up & has_left, 0), (has_up & has_right, 2),
            (has_down & has_left, 6), (has_down & has_right, 8),
        ]:
            @pl.when(has)
            def _(hood=hood, item=item):
                copy(own(item), hood, item, down).wait_recv()
    for item in order:
        to_down, to_up = (has_down & even, has_up & odd) if item == 0 else (has_down, has_up)
        for has, hood in [
            (has_right, 3), (has_left, 5), (has_down, 1), (has_up, 7),
            (to_down & has_left, 0), (to_up & has_left, 6),
            (to_down & has_right, 2), (to_up & has_right, 8),
        ]:
            @pl.when(has)
            def _(hood=hood, item=item):
                copy(own(item), hood, item, down).wait_send()
    for hood, has, to_right, to_left in outward:
        for side, target, device in ((has_right, to_right, right), (has_left, to_left, left)):
            @pl.when(has & side)
            def _(hood=hood, target=target, device=device):
                turned(hood, target, device).wait_send()
    for c in row_copies + col_copies:
        c.wait_send()
    swap.wait()


def exchange(rows, cols, vec, coords, skeleton, basis, transfer, device_skeleton):
    chunks = vec.shape[0] // CHUNK
    rank = basis.shape[0]
    vmem = pl.BlockSpec(memory_space=pltpu.VMEM)
    hbm = pl.BlockSpec(memory_space=pltpu.HBM)
    geo = (8, coords.shape[1] + skeleton.shape[1])
    coeff = (transfer.shape[1] // 2, 2 * vec.shape[0])
    share = (rank + 16, 128)
    dma = pltpu.SemaphoreType.DMA
    return pl.pallas_call(
        functools.partial(halo_kernel, rows, cols),
        out_shape=(
            jax.ShapeDtypeStruct((9, *vec.shape), BF16),
            jax.ShapeDtypeStruct((9, *geo), BF16),
            jax.ShapeDtypeStruct((9, *coeff), BF16),
            jax.ShapeDtypeStruct((2, cols, rows // 2, *share), BF16),
        ),
        in_specs=[vmem] * 6,
        out_specs=(hbm, hbm, hbm, vmem),
        scratch_shapes=[
            pltpu.VMEM(geo, BF16), pltpu.VMEM(coeff, BF16), pltpu.VMEM(share, BF16),
            pltpu.VMEM((rows, *share), BF16),
            dma((9, chunks + 2)), dma((9, chunks + 2)), dma((9,)),
            dma((rows,)), dma((rows,)), dma((cols,)), dma((cols,)), dma((4,)),
        ],
        compiler_params=pltpu.CompilerParams(
            collective_id=0, has_side_effects=True, vmem_limit_bytes=58 * 2**20
        ),
        name="halo",
    )(vec, coords, skeleton, basis, transfer, device_skeleton)


GROUP = 32
AHEAD = 4
RING = 64
STAGES = 4


def near_kernel(
    blocks, leaves, index, vec_pool, geo_pool,
    partial, mine, feats, vbuf, acc, stage, touched, vsem, gsem, ssem,
):
    width = vbuf.shape[2]
    count = 9 * leaves
    share = stage.shape[1]
    geo_copy = pltpu.make_async_copy(geo_pool, feats, gsem.at[0])
    geo_copy.start()

    def fetch(p, slot):
        hood, leaf = index[2, p], index[3, p]
        return pltpu.make_async_copy(
            vec_pool.at[hood, :, pl.ds(pl.multiple_of(leaf * width, width), width)], vbuf.at[slot], vsem.at[slot]
        )

    for p in range(RING):
        fetch(p, p).start()

    @pl.loop(0, count)
    def _(i):
        touched[i] = 0

    geo_copy.wait()

    def features(hood, leaf):
        return feats[hood, :, pl.ds(pl.multiple_of(leaf * width, width), width)].astype(F32)

    def power(p):
        tgt = features(index[0, p], index[1, p])
        src = features(index[2, p], index[3, p])
        left, right = left_rows(src).astype(BF16), right_rows(tgt).astype(BF16)
        return lax.dot_general(left, right, (((0,), (0,)), ((), ())), preferred_element_type=F32)

    @pl.loop(0, blocks // GROUP)
    def _(step):
        first = step * GROUP
        at = lax.rem(first, RING)
        for k in range(GROUP):
            fetch(first + k, at + k).wait()
        ahead = [power(first + k) for k in range(AHEAD)]
        for k in range(GROUP):
            now = ahead.pop(0)
            if k + AHEAD < GROUP:
                ahead.append(power(first + k + AHEAD))
            part = jnp.dot(vbuf[at + k], jnp.exp2(now).astype(BF16), preferred_element_type=F32)
            place = index[0, first + k] * leaves + index[1, first + k]
            seen = touched[place]
            touched[place] = 1
            acc[place] = jnp.where(seen > 0, acc[place], 0.0) + part

        @pl.when(first + RING < blocks)
        def _():
            for k in range(GROUP):
                fetch(first + RING + k, at + k).start()

    def settle(place):
        @pl.when(touched[place] == 0)
        def _():
            acc[place] = jnp.zeros(acc.shape[1:], F32)

    @pl.loop(0, leaves)
    def _(leaf):
        settle(4 * leaves + leaf)

    put_mine = pltpu.make_async_copy(acc.at[pl.ds(4 * leaves, leaves)], mine, gsem.at[0])
    put_mine.start()

    def put(hood, part):
        return pltpu.make_async_copy(
            stage.at[lax.rem(part, STAGES)], partial.at[hood, pl.ds(part * share, share)],
            ssem.at[lax.rem(part, STAGES)],
        )

    parts = leaves // share
    for hood in [h for h in range(9) if h != 4]:
        @pl.loop(0, parts)
        def _(part, hood=hood):
            if hood == 0:
                @pl.when(part >= STAGES)
                def _():
                    put(hood, part).wait()
            else:
                put(hood, part).wait()

            @pl.loop(0, share, unroll=4)
            def _(k):
                place = hood * leaves + part * share + k
                stage[lax.rem(part, STAGES), k] = jnp.where(touched[place] > 0, acc[place], 0.0).astype(BF16)

            put(hood, part).start()

    for slot in range(STAGES):
        put(0, slot).wait()
    put_mine.wait()


def near_blocks(index, vec_pool, geo_pool, leaves, width):
    blocks = index.shape[1]
    vecs = vec_pool.shape[1]
    share = leaves // STAGES
    hbm = pl.BlockSpec(memory_space=pl.ANY)
    dma = pltpu.SemaphoreType.DMA
    return pl.pallas_call(
        functools.partial(near_kernel, blocks, leaves),
        out_shape=(
            jax.ShapeDtypeStruct((9, leaves, vecs, width), BF16),
            jax.ShapeDtypeStruct((leaves, vecs, width), F32),
        ),
        in_specs=[pl.BlockSpec(memory_space=pltpu.SMEM), hbm, hbm],
        out_specs=(hbm, hbm),
        scratch_shapes=[
            pltpu.VMEM(geo_pool.shape, BF16),
            pltpu.VMEM((RING, vecs, width), BF16),
            pltpu.VMEM((9 * leaves, vecs, width), F32),
            pltpu.VMEM((STAGES, share, vecs, width), BF16),
            pltpu.SMEM((9 * leaves,), jnp.int32),
            dma((RING,)), dma((1,)), dma((STAGES,)),
        ],
        compiler_params=pltpu.CompilerParams(vmem_limit_bytes=58 * 2**20),
        name="near",
    )(index, vec_pool, geo_pool)


def left_rows(part):
    unit = lax.rem(lax.broadcasted_iota(jnp.int32, part.shape, 0), 4) == 3
    return jnp.concatenate([part, jnp.where(unit, 1.0, part)], axis=0)


def right_rows(part):
    row_id = lax.broadcasted_iota(jnp.int32, part.shape, 0)
    turned = jnp.concatenate([part[4:8], part[0:4]], axis=0)
    upper = jnp.where(lax.rem(row_id, 4) == 3, 1.0, jnp.where(row_id < 4, part, turned))
    return jnp.concatenate([upper, jnp.where(row_id < 3, turned, part)], axis=0)


def far_field(rank, far_index, top_index, own_top, coeff, skel, skel_rows, tops, turn, field, chunks):
    groups, vecs, lanes = field.shape
    members = lanes // rank
    partners = far_index.shape[1] // (groups * members)
    first_dim = (((0,), (0,)), ((), ()))
    lane = lax.broadcasted_iota(jnp.int32, (partners * rank, lanes), 1) // rank

    @pl.loop(0, 9)
    def _(hood):
        @pl.loop(0, groups)
        def _(q):
            part = skel[hood, :, pl.ds(pl.multiple_of(q * lanes, lanes), lanes)].astype(F32)
            turned = left_rows(part).T.astype(BF16)
            for member in range(members):
                skel_rows[(hood * groups + q) * members + member] = turned[member * rank : (member + 1) * rank]

    chosen = [tops[top_index[f]].astype(F32) for f in range(top_index.shape[0])]
    top = jnp.concatenate([c[:rank, :vecs] + c[:rank, vecs:] for c in chosen], axis=0)
    parts = jnp.concatenate([c[rank:].T[:rank] for c in chosen], axis=0)
    spots = parts[:, 0:3] + parts[:, 3:6] + parts[:, 6:9]
    total = None
    for k in range(3):
        gap = spots[:, k : k + 1] - own_top[k : k + 1, :]
        total = gap * gap if total is None else total + gap * gap
    device_far = lax.dot_general(
        top, jnp.exp(-0.5 * total), first_dim, precision=HIGH, preferred_element_type=F32
    )
    device_far = jnp.concatenate([device_far] * members, axis=1)
    square = lambda axis: lax.broadcasted_iota(jnp.int32, (lanes, lanes), axis) // rank
    same = square(0) == square(1)

    def part(c):
        @pl.loop(c * groups // chunks, (c + 1) * groups // chunks)
        def _(q):
            right = right_rows(skel[4, :, pl.ds(pl.multiple_of(q * lanes, lanes), lanes)].astype(F32)).astype(BF16)
            back = turn[:, pl.ds(pl.multiple_of(q * lanes, lanes), lanes)].T
            back = jnp.where(same, jnp.concatenate([back] * members, axis=1), 0.0)
            total = jnp.dot(device_far, back, precision=HIGH, preferred_element_type=F32)
            for member in range(members):
                lefts, coeffs = [], []
                for f in range(partners):
                    at = (q * members + member) * partners + f
                    lefts.append(skel_rows[far_index[0, at]])
                    both = coeff[far_index[1, at]]
                    odd = jnp.full((rank, vecs), far_index[2, at], jnp.int32) > 0
                    coeffs.append(jnp.where(odd, both[:, vecs:].astype(F32), both[:, :vecs].astype(F32)))
                left = jnp.concatenate(lefts, axis=0)
                picked = jnp.concatenate(coeffs, axis=0).astype(BF16)
                block = jnp.exp2(jnp.dot(left, right, preferred_element_type=F32))
                block = jnp.where(lane == member, block, 0.0)
                high = block.astype(BF16)
                low = (block - high.astype(F32)).astype(BF16)
                total += lax.dot_general(picked, high, first_dim, preferred_element_type=F32)
                total += lax.dot_general(picked, low, first_dim, preferred_element_type=F32)
            field[q] = total

    return part


def return_kernel(
    rows, cols, chunks, rank, far_index, top_index, own_top, partial, mine, coeff_pool, geo_pool, every, back, basis,
    out,
    from_rows, sums, from_cols, base, result, coeff, skel, skel_rows, tops, turn, base_rows, field, crossed, passing,
    row_send, row_recv, col_send, col_recv, cross_send, cross_recv, local, done,
):
    row, col = lax.axis_index("row"), lax.axis_index("col")
    has_row = (row > 0, row < rows - 1)
    has_col = (col > 0, col < cols - 1)
    leaves, vecs, width = base.shape
    share = leaves // chunks
    points = leaves * width
    parity = lax.rem(row, 2)
    leaving = (has_row[0] & (parity == 0), has_row[1] & (parity == 1))

    def side_of(place):
        return parity * 6 + place

    pairs = [
        (partial.at[3], sums.at[0]), (partial.at[5], sums.at[1]), (coeff_pool, coeff),
        (geo_pool.at[:, :, pl.ds(points, leaves * rank)], skel), (every, tops), (back, turn),
        (basis, base_rows), (mine, base), (partial.at[side_of(1), pl.ds(0, share)], passing),
    ]
    loads = [pltpu.make_async_copy(src, dst, local.at[n]) for n, (src, dst) in enumerate(pairs)]
    for c in loads:
        c.start()
    barrier = pltpu.get_barrier_semaphore()
    row_dev = ((row - 1, col), (row + 1, col))
    col_dev = ((row, col - 1), (row, col + 1))
    peers = 0
    for has, dev in zip(has_row + has_col, row_dev + col_dev):
        peers = peers + has.astype(jnp.int32)

        @pl.when(has)
        def _(dev=dev):
            pl.semaphore_signal(barrier, inc=1, device_id=dev, device_id_type=MESH)
    pl.semaphore_wait(barrier, peers)

    def some(c):
        return pl.ds(c * share, share)

    def row_copy(side, place, c, src=None):
        hood = (0 if side == 0 else 6) + (0, 2, 1)[place]
        return remote(
            partial.at[hood, some(c)] if src is None else src, from_rows.at[1 - side, place, some(c)],
            row_send.at[side, place, c], row_recv.at[1 - side, place, c], row_dev[side],
        )

    def col_copy(side, c):
        return remote(
            sums.at[side, some(c)], from_cols.at[1 - side, some(c)],
            col_send.at[side, c], col_recv.at[1 - side, c], col_dev[side],
        )

    def cross_copy(side):
        return remote(
            partial.at[side_of(2 * side), pl.ds(0, share)], crossed.at[1 - side],
            cross_send.at[side], cross_recv.at[1 - side], col_dev[side],
        )

    def put(c):
        part = pl.ds(c * share * width, share * width)
        return pltpu.make_async_copy(result.at[:, part], out.at[:, part], done.at[c])

    crossing = leaving[0] | leaving[1]
    for side in (0, 1):
        @pl.when(crossing & has_col[side])
        def _(side=side):
            cross_copy(side).start()

    def sent(side, place, c):
        if c > 0:
            return has_row[side] & (has_col[place] if place < 2 else True)
        stays = has_row[side] & (parity != side)
        return stays & has_col[place] if place < 2 else stays

    later = list(range(1, chunks))
    plan = [(place, 0) for place in (0, 1, 2)] + [(place, c) for c in later for place in (0, 1)]
    plan += [(2, c) for c in later]
    for place, c in plan:
        for side in (0, 1):
            @pl.when(sent(side, place, c))
            def _(side=side, place=place, c=c):
                row_copy(side, place, c).start()

    def fill(ref):
        @pl.loop(0, ref.shape[0])
        def _(i):
            ref[i] = jnp.zeros((vecs, width), BF16)

    for side in (0, 1):
        @pl.when(jnp.logical_not(has_row[side]))
        def _(side=side):
            for place in range(3):
                fill(from_rows.at[side, place])

        @pl.when(leaving[side])
        def _(side=side):
            for place in range(2):
                fill(from_rows.at[side, place, pl.ds(0, share)])

        @pl.when(jnp.logical_not(has_col[side]))
        def _(side=side):
            fill(from_cols.at[side])
            fill(crossed.at[side])

    for c in loads:
        c.wait()
    parts = far_field(rank, far_index, top_index, own_top, coeff, skel, skel_rows, tops, turn, field, chunks)

    @pl.when(crossing)
    def _():
        for side in (0, 1):
            @pl.when(has_col[side])
            def _(side=side):
                cross_copy(1 - side).wait_recv()

        @pl.loop(0, share)
        def _(i):
            total = passing[i].astype(F32) + crossed[0, i].astype(F32) + crossed[1, i].astype(F32)
            passing[i] = total.astype(BF16)

        for side in (0, 1):
            @pl.when(leaving[side])
            def _(side=side):
                row_copy(side, 2, 0, passing).start()

    for c in range(chunks):
        for place in (0, 1):
            @pl.when(has_col[place])
            def _(place=place, c=c):
                for side in (0, 1):
                    @pl.when(has_row[side] if c > 0 else has_row[side] & (parity != side))
                    def _(side=side):
                        row_copy(1 - side, place, c).wait_recv()

                @pl.loop(c * share, (c + 1) * share)
                def _(i):
                    total = (
                        sums[place, i].astype(F32)
                        + from_rows[0, place, i].astype(F32)
                        + from_rows[1, place, i].astype(F32)
                    )
                    sums[place, i] = total.astype(BF16)

                col_copy(place, c).start()

        parts(c)

    for c in range(chunks):
        for side in (0, 1):
            @pl.when(has_row[side])
            def _(side=side, c=c):
                row_copy(1 - side, 2, c).wait_recv()

            @pl.when(has_col[side])
            def _(side=side, c=c):
                col_copy(1 - side, c).wait_recv()

        group = 128 // rank
        lane = lax.broadcasted_iota(jnp.int32, (vecs, 128), 1) // rank

        @pl.loop(c * share, (c + 1) * share)
        def _(i):
            points_of = pl.ds(pl.multiple_of(i * width, width), width)
            weights = jnp.where(lane == lax.rem(i, group), field[i // group], 0.0).astype(BF16)
            spread = jnp.concatenate([base_rows[:, points_of]] * group, axis=0)
            result[:, points_of] = (
                jnp.dot(weights, spread, preferred_element_type=F32)
                + base[i]
                + from_rows[0, 2, i].astype(F32)
                + from_rows[1, 2, i].astype(F32)
                + from_cols[0, i].astype(F32)
                + from_cols[1, i].astype(F32)
            )

        put(c).start()

    for place, c in plan:
        for side in (0, 1):
            @pl.when(sent(side, place, c))
            def _(side=side, place=place, c=c):
                row_copy(side, place, c).wait_send()
    for side in (0, 1):
        @pl.when(leaving[side])
        def _(side=side):
            row_copy(side, 2, 0, passing).wait_send()

        @pl.when(crossing & has_col[side])
        def _(side=side):
            cross_copy(side).wait_send()
    for c in range(chunks):
        for side in (0, 1):
            @pl.when(has_col[side])
            def _(side=side, c=c):
                col_copy(side, c).wait_send()
    for c in range(chunks):
        put(c).wait()


def give_back(rows, cols, far_index, top_index, own_top, partial, mine, coeff_pool, geo_pool, every, back, basis):
    leaves, vecs, width = mine.shape
    rank = basis.shape[0]
    chunks = math.gcd(leaves, 4)
    vmem, smem = pl.BlockSpec(memory_space=pltpu.VMEM), pl.BlockSpec(memory_space=pltpu.SMEM)
    hbm = pl.BlockSpec(memory_space=pltpu.HBM)
    dma = pltpu.SemaphoreType.DMA
    return pl.pallas_call(
        functools.partial(return_kernel, rows, cols, chunks, rank),
        out_shape=jax.ShapeDtypeStruct((vecs, leaves * width), F32),
        in_specs=[smem, smem, vmem] + [hbm] * 7,
        out_specs=hbm,
        scratch_shapes=[
            pltpu.VMEM((2, 3, leaves, vecs, width), BF16),
            pltpu.VMEM((2, leaves, vecs, width), BF16),
            pltpu.VMEM((2, leaves, vecs, width), BF16),
            pltpu.VMEM(mine.shape, F32),
            pltpu.VMEM((vecs, leaves * width), F32),
            pltpu.VMEM(coeff_pool.shape, BF16),
            pltpu.VMEM((9, 8, leaves * rank), BF16),
            pltpu.VMEM((9 * leaves, rank, 16), BF16),
            pltpu.VMEM(every.shape, BF16),
            pltpu.VMEM(back.shape, F32),
            pltpu.VMEM(basis.shape, BF16),
            pltpu.VMEM((leaves * rank // 128, vecs, 128), F32),
            pltpu.VMEM((2, leaves // chunks, vecs, width), BF16),
            pltpu.VMEM((leaves // chunks, vecs, width), BF16),
            dma((2, 3, chunks)), dma((2, 3, chunks)), dma((2, chunks)), dma((2, chunks)), dma((2,)), dma((2,)), dma((9,)), dma((chunks,)),
        ],
        compiler_params=pltpu.CompilerParams(
            collective_id=1, has_side_effects=True, vmem_limit_bytes=56 * 2**20
        ),
        name="give_back",
    )(far_index, top_index, own_top, partial, mine, coeff_pool, geo_pool, every, back, basis)


def shards(
    coords, vectors, basis, transfer, leaf_skeleton, device_skeleton, near_pairs, far_leaves, far_devices
):
    row_count, col_count = lax.axis_size("row"), lax.axis_size("col")
    row_here, col_here = lax.axis_index("row"), lax.axis_index("col")
    rank_size, vec_count = basis.shape[0], vectors.shape[0]
    leaves = transfer.shape[1] // rank_size
    leaf_width = coords.shape[1] // leaves

    def hood_of(global_leaf):
        owner = global_leaf // leaves
        hood = (owner // col_count - row_here + 1) * 3 + (owner % col_count - col_here + 1)
        return hood, global_leaf % leaves

    vec_pool, geo_pool, coeff_pool, every = exchange(
        row_count, col_count, vectors, coords, leaf_skeleton, basis, transfer, device_skeleton
    )

    t_hood, t_leaf = hood_of(near_pairs[0])
    s_hood, s_leaf = hood_of(near_pairs[1])
    index = jnp.stack([t_hood, t_leaf, s_hood, s_leaf])
    partial, mine = near_blocks(index, vec_pool, geo_pool, leaves, leaf_width)

    far_hood, far_leaf = hood_of(far_leaves.reshape(-1))
    far_place = far_hood * leaves + far_leaf
    far_index = jnp.stack([far_place, far_place // 2, far_place % 2])
    chosen = far_devices[0]
    rows_half = row_count // 2
    top_row, top_col = chosen // col_count, chosen % col_count
    top_index = (top_row // rows_half * col_count + top_col) * rows_half + top_row % rows_half
    return give_back(
        row_count, col_count, far_index, top_index, device_skeleton,
        partial, mine, coeff_pool.reshape(-1, rank_size, 2 * vec_count), geo_pool,
        every.reshape(-1, *every.shape[3:]), transfer, basis,
    )


def solution(mesh):
    wide = P(None, ("row", "col"))
    tall = P(("row", "col"), None)
    return jax.shard_map(
        shards, mesh=mesh, in_specs=(wide,) * 7 + (tall,) * 2, out_specs=wide, check_vma=False
    )
```
